16 devices in a mesh: dp: 16 (over z, y, x, core).
Axes of the slice: x: 2, y: 2, z: 2, core: 2. Of those that a mesh axis runs over, the one named last changes fastest.
Arguments:
- local_grads: bfloat16 [16, 32768, 768], P('dp')
- master: float32 [32768, 768], P('dp')
- mom_first: float32 [32768, 768], P('dp')
- mom_second: float32 [32768, 768], P('dp')
- learn_rate: float32 [], replicated
Outputs:
- output 1: float32 [32768, 768], P('dp')
- output 2: float32 [32768, 768], P('dp')
- output 3: float32 [32768, 768], P('dp')
- output 4: bfloat16 [32768, 768], replicated
All inputs are finite; a program needn't handle non-finite values.
Results may differ from the reference program's by a relative error of at most 0.001.
Values are sent between devices in bfloat16 or wider.
A program may use at most 1 GiB of HBM per device.

```python
import math
import jax
import jax.numpy as jnp
import numpy as np
from jax import lax

D = 768
ROWS_DEV = 2048
DEVICES = 16
LAYERS = 2
MIX_RANK = 32
DECAY_RANK = 64
ADAM_STEP = 10


def rule_table(model_width, total_rows):
    ffn_width = 7 * model_width // 2
    layer_rows = 6 * model_width + 2 * ffn_width + 16 + 10 * MIX_RANK + 2 * DECAY_RANK
    vocab_rows = (total_rows - LAYERS * layer_rows - 4) // 2
    base_rule = (1.0, 0.0)
    decay_rule = (1.0, 0.1)
    time_rule = (2.0, 0.0)
    pieces = [(vocab_rows, decay_rule)]
    for layer_idx in range(LAYERS):
        lead_rows = 12 if layer_idx == 0 else 10
        pieces = pieces + [(lead_rows + 10 * MIX_RANK, base_rule), (1, time_rule), (2 * DECAY_RANK, base_rule), (1, time_rule), (5 * model_width, decay_rule), (4, base_rule), (2 * ffn_width + model_width, decay_rule)]
    pieces = pieces + [(2, base_rule), (vocab_rows, decay_rule)]
    run_lengths = np.array([run_len for run_len, run_rule in pieces])
    lr_factor = np.repeat(np.array([run_rule[0] for run_len, run_rule in pieces]), run_lengths)
    decay_rate = np.repeat(np.array([run_rule[1] for run_len, run_rule in pieces]), run_lengths)
    return lr_factor, decay_rate


def setup_inputs(seed: int = 0) -> dict:
    key_grad, key_master, key_first, key_second, key_rate = jax.random.split(jax.random.key(seed), 5)
    total_rows = DEVICES * ROWS_DEV
    elem_count = total_rows * D
    grad_scale = 3.0 * math.sqrt(DEVICES / elem_count)
    clip_unit = 1.0 / math.sqrt(elem_count)

    def draw_device(dev_key):
        gauss_noise = jax.random.normal(dev_key, (total_rows, D), jnp.float32)
        return (grad_scale * gauss_noise).astype(jnp.bfloat16)

    local_grads = lax.map(draw_device, jax.random.split(key_grad, DEVICES))
    master = (0.5 / math.sqrt(D)) * jax.random.normal(key_master, (total_rows, D), jnp.float32)
    mom_first = 0.1 * clip_unit * jax.random.normal(key_first, (total_rows, D), jnp.float32)
    mom_second = jnp.square(0.1 * clip_unit * jax.random.uniform(key_second, (total_rows, D), jnp.float32, 0.5, 1.5))
    learn_rate = jax.random.uniform(key_rate, (), jnp.float32, 0.005, 0.015)
    return {'local_grads': local_grads, 'master': master, 'mom_first': mom_first, 'mom_second': mom_second, 'learn_rate': learn_rate}


def reference(local_grads, master, mom_first, mom_second, learn_rate):
    def add_device(running, grad_block):
        return running + grad_block.astype(jnp.float32), None

    grad_total = lax.scan(add_device, jnp.zeros(master.shape, jnp.float32), local_grads)[0]
    grad_mean = grad_total / local_grads.shape[0]
    grad_norm = jnp.sqrt(jnp.sum(grad_mean * grad_mean))
    clip_scale = jnp.minimum(1.0, 1.0 / (grad_norm + 1e-6))
    clipped = grad_mean * clip_scale
    new_first = 0.9 * mom_first + 0.1 * clipped
    new_second = 0.99 * mom_second + 0.01 * (clipped * clipped)
    first_hat = new_first / (1.0 - 0.9 ** ADAM_STEP)
    second_hat = new_second / (1.0 - 0.99 ** ADAM_STEP)
    lr_factor, decay_rate = rule_table(master.shape[1], master.shape[0])
    row_rate = learn_rate * jnp.asarray(lr_factor, jnp.float32)[:, None]
    row_decay = jnp.asarray(decay_rate, jnp.float32)[:, None]
    new_master = master - row_rate * (first_hat / (jnp.sqrt(second_hat) + 1e-8) + row_decay * master)
    return new_master, new_first, new_second, new_master.astype(jnp.bfloat16)
```

```python
import functools

import jax
import jax.numpy as jnp
from jax import lax
from jax.experimental import pallas as pl
from jax.experimental.pallas import tpu as pltpu
from jax.sharding import PartitionSpec as P

LAYERS = 2
MIX_RANK = 32
DECAY_RANK = 64
ADAM_STEP = 10

AXES = 3
CHUNKS = 4
SLOTS = 3
MESH = pl.DeviceIdType.MESH


def layout_runs(model_width, total_rows):
    ffn_width = 7 * model_width // 2
    layer_rows = 6 * model_width + 2 * ffn_width + 16 + 10 * MIX_RANK + 2 * DECAY_RANK
    vocab_rows = (total_rows - LAYERS * layer_rows - 4) // 2
    base_rule = (1.0, 0.0)
    decay_rule = (1.0, 0.1)
    time_rule = (2.0, 0.0)
    pieces = [(vocab_rows, decay_rule)]
    for layer_idx in range(LAYERS):
        lead_rows = 12 if layer_idx == 0 else 10
        pieces = pieces + [(lead_rows + 10 * MIX_RANK, base_rule), (1, time_rule), (2 * DECAY_RANK, base_rule), (1, time_rule), (5 * model_width, decay_rule), (4, base_rule), (2 * ffn_width + model_width, decay_rule)]
    pieces = pieces + [(2, base_rule), (vocab_rows, decay_rule)]
    run_starts = []
    next_row = 0
    for run_len, run_rule in pieces:
        run_starts.append(next_row)
        next_row = next_row + run_len
    lr_values = [run_rule[0] for run_len, run_rule in pieces]
    decay_values = [run_rule[1] for run_len, run_rule in pieces]
    return run_starts, lr_values, decay_values


def row_rules(row_ids, model_width, total_rows):
    run_starts, lr_values, decay_values = layout_runs(model_width, total_rows)
    later_starts = jnp.asarray(run_starts[1:], jnp.int32)
    run_index = jnp.sum((row_ids[:, None] >= later_starts[None, :]).astype(jnp.int32), axis=1)
    lr_factor = jnp.asarray(lr_values, jnp.float32)[run_index]
    decay_rate = jnp.asarray(decay_values, jnp.float32)[run_index]
    return lr_factor[:, None], decay_rate[:, None]


def adam_rows(grad_rows, master_rows, first_rows, second_rows, clip_scale, learn_rate, lr_factor, decay_rate):
    clipped = grad_rows * clip_scale
    new_first = 0.9 * first_rows + 0.1 * clipped
    new_second = 0.99 * second_rows + 0.01 * (clipped * clipped)
    first_hat = new_first / (1.0 - 0.9 ** ADAM_STEP)
    second_hat = new_second / (1.0 - 0.99 ** ADAM_STEP)
    step_size = learn_rate * lr_factor
    new_master = master_rows - step_size * (first_hat / (jnp.sqrt(second_hat) + 1e-8) + decay_rate * master_rows)
    return new_master, new_first, new_second


def bit_flip(index, mask):
    flipped = index
    for bit in range(4):
        step = 1 << bit
        if mask & step:
            flipped = flipped + step - 2 * step * ((index // step) % 2)
    return flipped


def dest_mask(e, k):
    mask = 0
    for place in range(AXES):
        if e >> (2 - place) & 1:
            mask |= 1 << ((k + place) % AXES)
    return mask


def reduce_kernel(grads, g_out, c_out, pairs, landed, stage, own_buf, pair_buf, part_buf, norm_buf,
                  pair_ssem, pair_rsem, send_sem, recv_sem, own_sem, pairl_sem, norm_ssem, norm_rsem, g_sem):
    me = lax.axis_index('dp')
    chip, core = me // 2, me % 2
    partner = bit_flip(me, 1)
    rows = g_out.shape[0]
    third = g_out.shape[1] // AXES
    part_rows = rows // CHUNKS
    devices = norm_buf.shape[0]

    def unit_row(j, k, parity):
        row = 0
        flip = chip
        e = 7 - j
        for place in range(AXES):
            step = 1 << ((k + place) % AXES)
            want = (e // (1 << (2 - place))) % 2
            bit = (chip // step) % 2
            flip = flip + want * (step - 2 * step * bit)
        return (2 * flip + parity) * rows + row

    def pair_copy(j, k):
        return pltpu.make_async_remote_copy(
            src_ref=grads.at[0, pl.ds(pl.multiple_of(unit_row(j, k, 1 - core), rows), rows), pl.ds(k * third, third)],
            dst_ref=pairs.at[j, k],
            send_sem=pair_ssem.at[j, k],
            recv_sem=pair_rsem.at[j, k],
            device_id=(partner,),
            device_id_type=MESH)

    def own_load(s, k):
        j, i = s // CHUNKS, s % CHUNKS
        row = pl.multiple_of(unit_row(j, k, core) + i * part_rows, part_rows)
        return pltpu.make_async_copy(
            grads.at[0, pl.ds(row, part_rows), pl.ds(k * third, third)], own_buf.at[s % 2, k], own_sem.at[s % 2, k])

    def pair_load(s, k):
        j, i = s // CHUNKS, s % CHUNKS
        return pltpu.make_async_copy(
            pairs.at[j, k, pl.ds(pl.multiple_of(i * part_rows, part_rows), part_rows)], pair_buf.at[s % 2, k], pairl_sem.at[s % 2, k])

    def piece_copy(j, i, k, slot, axis):
        return pltpu.make_async_remote_copy(
            src_ref=stage.at[k, slot],
            dst_ref=landed.at[j, k, pl.ds(pl.multiple_of(i * part_rows, part_rows), part_rows)],
            send_sem=send_sem.at[k, slot],
            recv_sem=recv_sem.at[j, k, i],
            device_id=(bit_flip(me, 2 << axis),),
            device_id_type=MESH)

    def start_loads(s):
        for k in range(AXES):
            @pl.when(s % CHUNKS == 0)
            def _():
                pair_copy(s // CHUNKS, k).wait_recv()
            own_load(s, k).start()
            pair_load(s, k).start()

    for j in range(8):
        for k in range(AXES):
            pair_copy(j, k).start()

    total_steps = 8 * CHUNKS
    start_loads(0)

    def step(s, phase):
        j, i = s // CHUNKS, s % CHUNKS

        @pl.when(s + 1 < total_steps)
        def _():
            start_loads(s + 1)

        if phase == 1:
            sources = []
        elif phase == 2:
            sources = [j - 4]
        elif phase == 3:
            sources = [2, 4]
        else:
            sources = [3, 5, 6]
        slot = s % SLOTS
        base = pl.multiple_of(i * part_rows, part_rows)
        for k in range(AXES):
            own_load(s, k).wait()
            pair_load(s, k).wait()
            for source in sources:
                piece_copy(source, i, k, 0, 0).wait_recv()
            if phase < 4:
                @pl.when(s >= SLOTS)
                def _():
                    piece_copy(0, 0, k, slot, 0).wait_send()
            group = 64

            def add_rows(r, carry):
                lo = pl.multiple_of(r * group, group)
                value = own_buf[s % 2, k, pl.ds(lo, group)].astype(jnp.float32) + pair_buf[s % 2, k, pl.ds(lo, group)].astype(jnp.float32)
                for source in sources:
                    value = value + landed[source, k, pl.ds(base + lo, group)]
                if phase < 4:
                    stage[k, slot, pl.ds(lo, group)] = value
                    return carry
                value = value * (1.0 / devices)
                landed[0, k, pl.ds(base + lo, group)] = value
                return carry + jnp.sum((value * value).reshape(group // 8, 8, third), axis=0)

            if phase < 4:
                lax.fori_loop(0, part_rows // group, add_rows, 0)
            else:
                part_buf[...] += lax.fori_loop(0, part_rows // group, add_rows, jnp.zeros((8, third), jnp.float32))
        for k in range(AXES):
            if phase < 4:
                piece_copy(j, i, k, slot, (k + phase - 1) % AXES).start()
            else:
                pltpu.make_async_copy(
                    landed.at[0, k, pl.ds(base, part_rows)],
                    g_out.at[pl.ds(base, part_rows), pl.ds(k * third, third)], g_sem.at[k, i]).start()

    part_buf[...] = jnp.zeros_like(part_buf)
    for phase, lo, hi in ((1, 0, 4), (2, 4, 6), (3, 6, 7), (4, 7, 8)):
        def run(s, carry, phase=phase):
            step(s, phase)
            return carry
        lax.fori_loop(lo * CHUNKS, hi * CHUNKS, run, 0)

    part_buf[:, :128] = part_buf[:, :128] + part_buf[:, 128:]
    norm_buf[me] = part_buf[:, :128]

    def norm_copy(d):
        return pltpu.make_async_remote_copy(
            src_ref=part_buf.at[:, pl.ds(0, 128)],
            dst_ref=norm_buf.at[me],
            send_sem=norm_ssem.at[d],
            recv_sem=norm_rsem.at[me],
            device_id=((me + d) % devices,),
            device_id_type=MESH)

    def norm_recv(d):
        sender = (me + devices - d) % devices
        return pltpu.make_async_remote_copy(
            src_ref=part_buf.at[:, pl.ds(0, 128)],
            dst_ref=norm_buf.at[sender],
            send_sem=norm_ssem.at[d],
            recv_sem=norm_rsem.at[sender],
            device_id=(partner,),
            device_id_type=MESH)

    for d in range(1, devices):
        norm_copy(d).start()
    for last in range(SLOTS):
        for k in range(AXES):
            piece_copy(0, 0, k, last, 0).wait_send()
    for j in range(8):
        for k in range(AXES):
            pair_copy(j, k).wait_send()
    for i in range(CHUNKS):
        for k in range(AXES):
            pltpu.make_async_copy(
                landed.at[0, k, pl.ds(i * part_rows, part_rows)],
                g_out.at[pl.ds(i * part_rows, part_rows), pl.ds(k * third, third)], g_sem.at[k, i]).wait()
    for d in range(1, devices):
        norm_copy(d).wait_send()
    for d in range(1, devices):
        norm_recv(d).wait_recv()
    square_sum = jnp.sum(jnp.sum(norm_buf[...], axis=0), keepdims=True)
    c_out[...] = jnp.broadcast_to(jnp.minimum(1.0, 1.0 / (jnp.sqrt(square_sum) + 1e-6)), c_out.shape)


def reduce_scatter(local_grads, devices):
    total_rows, width = local_grads.shape[1:]
    rows, third = total_rows // devices, width // AXES
    any_spec = pl.BlockSpec(memory_space=pl.ANY)
    f32, bf16 = jnp.float32, jnp.bfloat16
    part_rows = rows // CHUNKS
    g, scale, _ = pl.pallas_call(
        reduce_kernel,
        out_shape=(jax.ShapeDtypeStruct((rows, width), f32),
                   jax.ShapeDtypeStruct((8, 128), f32),
                   jax.ShapeDtypeStruct((8, AXES, rows, third), bf16)),
        in_specs=[any_spec],
        out_specs=(any_spec, pl.BlockSpec(memory_space=pltpu.VMEM), any_spec),
        scratch_shapes=[
            pltpu.VMEM((7, AXES, rows, third), f32),
            pltpu.VMEM((AXES, SLOTS, part_rows, third), f32),
            pltpu.VMEM((2, AXES, part_rows, third), bf16),
            pltpu.VMEM((2, AXES, part_rows, third), bf16),
            pltpu.VMEM((8, third), f32),
            pltpu.VMEM((devices, 8, 128), f32),
            pltpu.SemaphoreType.DMA((8, AXES)),
            pltpu.SemaphoreType.DMA((8, AXES)),
            pltpu.SemaphoreType.DMA((AXES, SLOTS)),
            pltpu.SemaphoreType.DMA((7, AXES, CHUNKS)),
            pltpu.SemaphoreType.DMA((2, AXES)),
            pltpu.SemaphoreType.DMA((2, AXES)),
            pltpu.SemaphoreType.DMA((devices,)),
            pltpu.SemaphoreType.DMA((devices,)),
            pltpu.SemaphoreType.DMA((AXES, CHUNKS)),
        ],
        compiler_params=pltpu.CompilerParams(has_side_effects=True, vmem_limit_bytes=60 * 1024 * 1024),
        name='reduce',
    )(local_grads)
    return g, scale[0, 0]


def solution(mesh):
    dev_count = mesh.shape['dp']

    def device_step(local_grads, master, mom_first, mom_second, learn_rate):
        shard_rows = master.shape[0]
        model_width = master.shape[1]
        total_rows = shard_rows * dev_count
        grad_shard, clip_scale = reduce_scatter(local_grads, dev_count)
        row_ids = lax.axis_index('dp') * shard_rows + lax.iota(jnp.int32, shard_rows)
        lr_factor, decay_rate = row_rules(row_ids, model_width, total_rows)
        new_master, new_first, new_second = adam_rows(grad_shard, master, mom_first, mom_second, clip_scale, learn_rate, lr_factor, decay_rate)
        working = lax.all_gather(new_master.astype(jnp.bfloat16), 'dp', axis=0, tiled=True)
        return new_master, new_first, new_second, working

    return jax.shard_map(device_step, mesh=mesh, in_specs=(P('dp', None, None), P('dp', None), P('dp', None), P('dp', None), P()), out_specs=(P('dp', None), P('dp', None), P('dp', None), P(None, None)), check_vma=False)
```

```python
import functools

import jax
import jax.numpy as jnp
from jax import lax
from jax.experimental import pallas as pl
from jax.experimental.pallas import tpu as pltpu
from jax.sharding import PartitionSpec as P

LAYERS = 2
MIX_RANK = 32
DECAY_RANK = 64
ADAM_STEP = 10

AXES = 3
CHUNKS = 4
SLOTS = 3
PIECE_ROWS = 256
MESH = pl.DeviceIdType.MESH


def layout_runs(model_width, total_rows):
    ffn_width = 7 * model_width // 2
    layer_rows = 6 * model_width + 2 * ffn_width + 16 + 10 * MIX_RANK + 2 * DECAY_RANK
    vocab_rows = (total_rows - LAYERS * layer_rows - 4) // 2
    base_rule = (1.0, 0.0)
    decay_rule = (1.0, 0.1)
    time_rule = (2.0, 0.0)
    pieces = [(vocab_rows, decay_rule)]
    for layer_idx in range(LAYERS):
        lead_rows = 12 if layer_idx == 0 else 10
        pieces = pieces + [(lead_rows + 10 * MIX_RANK, base_rule), (1, time_rule), (2 * DECAY_RANK, base_rule), (1, time_rule), (5 * model_width, decay_rule), (4, base_rule), (2 * ffn_width + model_width, decay_rule)]
    pieces = pieces + [(2, base_rule), (vocab_rows, decay_rule)]
    run_starts = []
    next_row = 0
    for run_len, run_rule in pieces:
        run_starts.append(next_row)
        next_row = next_row + run_len
    lr_values = [run_rule[0] for run_len, run_rule in pieces]
    decay_values = [run_rule[1] for run_len, run_rule in pieces]
    return run_starts, lr_values, decay_values


def bit_flip(index, mask):
    flipped = index
    for bit in range(4):
        step = 1 << bit
        if mask & step:
            flipped = flipped + step - 2 * step * ((index // step) % 2)
    return flipped


def reduce_kernel(grads, g_out, c_out, pairs, landed, stage, own_buf, pair_buf, part_buf, norm_buf,
                  pair_ssem, pair_rsem, send_sem, recv_sem, own_sem, pairl_sem, norm_ssem, norm_rsem, g_sem):
    me = lax.axis_index('dp')
    chip, core = me // 2, me % 2
    partner = bit_flip(me, 1)
    rows = g_out.shape[0]
    third = g_out.shape[1] // AXES
    part_rows = rows // CHUNKS
    devices = norm_buf.shape[0]

    def unit_row(j, k, parity):
        row = 0
        flip = chip
        e = 7 - j
        for place in range(AXES):
            step = 1 << ((k + place) % AXES)
            want = (e // (1 << (2 - place))) % 2
            bit = (chip // step) % 2
            flip = flip + want * (step - 2 * step * bit)
        return (2 * flip + parity) * rows + row

    def pair_copy(j, k):
        return pltpu.make_async_remote_copy(
            src_ref=grads.at[0, pl.ds(pl.multiple_of(unit_row(j, k, 1 - core), rows), rows), pl.ds(k * third, third)],
            dst_ref=pairs.at[j, k],
            send_sem=pair_ssem.at[j, k],
            recv_sem=pair_rsem.at[j, k],
            device_id=(partner,),
            device_id_type=MESH)

    def own_load(s, k):
        j, i = s // CHUNKS, s % CHUNKS
        row = pl.multiple_of(unit_row(j, k, core) + i * part_rows, part_rows)
        return pltpu.make_async_copy(
            grads.at[0, pl.ds(row, part_rows), pl.ds(k * third, third)], own_buf.at[s % 2, k], own_sem.at[s % 2, k])

    def pair_load(s, k):
        j, i = s // CHUNKS, s % CHUNKS
        return pltpu.make_async_copy(
            pairs.at[j, k, pl.ds(pl.multiple_of(i * part_rows, part_rows), part_rows)], pair_buf.at[s % 2, k], pairl_sem.at[s % 2, k])

    def piece_copy(j, i, k, slot, axis):
        return pltpu.make_async_remote_copy(
            src_ref=stage.at[k, slot],
            dst_ref=landed.at[j, k, pl.ds(pl.multiple_of(i * part_rows, part_rows), part_rows)],
            send_sem=send_sem.at[k, slot],
            recv_sem=recv_sem.at[j, k, i],
            device_id=(bit_flip(me, 2 << axis),),
            device_id_type=MESH)

    def start_loads(s):
        for k in range(AXES):
            @pl.when(s % CHUNKS == 0)
            def _():
                pair_copy(s // CHUNKS, k).wait_recv()
            own_load(s, k).start()
            pair_load(s, k).start()

    for j in range(8):
        for k in range(AXES):
            pair_copy(j, k).start()

    total_steps = 8 * CHUNKS
    start_loads(0)

    def step(s, phase):
        j, i = s // CHUNKS, s % CHUNKS

        @pl.when(s + 1 < total_steps)
        def _():
            start_loads(s + 1)

        if phase == 1:
            sources = []
        elif phase == 2:
            sources = [j - 4]
        elif phase == 3:
            sources = [2, 4]
        else:
            sources = [3, 5, 6]
        slot = s % SLOTS
        base = pl.multiple_of(i * part_rows, part_rows)
        for k in range(AXES):
            own_load(s, k).wait()
            pair_load(s, k).wait()
            for source in sources:
                piece_copy(source, i, k, 0, 0).wait_recv()
            if phase < 4:
                @pl.when(s >= SLOTS)
                def _():
                    piece_copy(0, 0, k, slot, 0).wait_send()
            group = 64

            def add_rows(r, carry):
                lo = pl.multiple_of(r * group, group)
                value = own_buf[s % 2, k, pl.ds(lo, group)].astype(jnp.float32) + pair_buf[s % 2, k, pl.ds(lo, group)].astype(jnp.float32)
                for source in sources:
                    value = value + landed[source, k, pl.ds(base + lo, group)]
                if phase < 4:
                    stage[k, slot, pl.ds(lo, group)] = value
                    return carry
                value = value * (1.0 / devices)
                landed[0, k, pl.ds(base + lo, group)] = value
                return carry + jnp.sum((value * value).reshape(group // 8, 8, third), axis=0)

            if phase < 4:
                lax.fori_loop(0, part_rows // group, add_rows, 0)
            else:
                part_buf[...] += lax.fori_loop(0, part_rows // group, add_rows, jnp.zeros((8, third), jnp.float32))
        for k in range(AXES):
            if phase < 4:
                piece_copy(j, i, k, slot, (k + phase - 1) % AXES).start()
            else:
                pltpu.make_async_copy(
                    landed.at[0, k, pl.ds(base, part_rows)],
                    g_out.at[pl.ds(base, part_rows), pl.ds(k * third, third)], g_sem.at[k, i]).start()

    part_buf[...] = jnp.zeros_like(part_buf)
    for phase, lo, hi in ((1, 0, 4), (2, 4, 6), (3, 6, 7), (4, 7, 8)):
        def run(s, carry, phase=phase):
            step(s, phase)
            return carry
        lax.fori_loop(lo * CHUNKS, hi * CHUNKS, run, 0)

    part_buf[:, :128] = part_buf[:, :128] + part_buf[:, 128:]
    norm_buf[me] = part_buf[:, :128]

    def norm_copy(d):
        return pltpu.make_async_remote_copy(
            src_ref=part_buf.at[:, pl.ds(0, 128)],
            dst_ref=norm_buf.at[me],
            send_sem=norm_ssem.at[d],
            recv_sem=norm_rsem.at[me],
            device_id=((me + d) % devices,),
            device_id_type=MESH)

    def norm_recv(d):
        sender = (me + devices - d) % devices
        return pltpu.make_async_remote_copy(
            src_ref=part_buf.at[:, pl.ds(0, 128)],
            dst_ref=norm_buf.at[sender],
            send_sem=norm_ssem.at[d],
            recv_sem=norm_rsem.at[sender],
            device_id=(partner,),
            device_id_type=MESH)

    for d in range(1, devices):
        norm_copy(d).start()
    for last in range(SLOTS):
        for k in range(AXES):
            piece_copy(0, 0, k, last, 0).wait_send()
    for j in range(8):
        for k in range(AXES):
            pair_copy(j, k).wait_send()
    for i in range(CHUNKS):
        for k in range(AXES):
            pltpu.make_async_copy(
                landed.at[0, k, pl.ds(i * part_rows, part_rows)],
                g_out.at[pl.ds(i * part_rows, part_rows), pl.ds(k * third, third)], g_sem.at[k, i]).wait()
    for d in range(1, devices):
        norm_copy(d).wait_send()
    for d in range(1, devices):
        norm_recv(d).wait_recv()
    square_sum = jnp.sum(jnp.sum(norm_buf[...], axis=0), keepdims=True)
    c_out[...] = jnp.broadcast_to(jnp.minimum(1.0, 1.0 / (jnp.sqrt(square_sum) + 1e-6)), c_out.shape)


def reduce_scatter(local_grads, devices):
    total_rows, width = local_grads.shape[1:]
    rows, third = total_rows // devices, width // AXES
    any_spec = pl.BlockSpec(memory_space=pl.ANY)
    f32, bf16 = jnp.float32, jnp.bfloat16
    part_rows = rows // CHUNKS
    g, scale, _ = pl.pallas_call(
        reduce_kernel,
        out_shape=(jax.ShapeDtypeStruct((rows, width), f32),
                   jax.ShapeDtypeStruct((8, 128), f32),
                   jax.ShapeDtypeStruct((8, AXES, rows, third), bf16)),
        in_specs=[any_spec],
        out_specs=(any_spec, pl.BlockSpec(memory_space=pltpu.VMEM), any_spec),
        scratch_shapes=[
            pltpu.VMEM((7, AXES, rows, third), f32),
            pltpu.VMEM((AXES, SLOTS, part_rows, third), f32),
            pltpu.VMEM((2, AXES, part_rows, third), bf16),
            pltpu.VMEM((2, AXES, part_rows, third), bf16),
            pltpu.VMEM((8, third), f32),
            pltpu.VMEM((devices, 8, 128), f32),
            pltpu.SemaphoreType.DMA((8, AXES)),
            pltpu.SemaphoreType.DMA((8, AXES)),
            pltpu.SemaphoreType.DMA((AXES, SLOTS)),
            pltpu.SemaphoreType.DMA((7, AXES, CHUNKS)),
            pltpu.SemaphoreType.DMA((2, AXES)),
            pltpu.SemaphoreType.DMA((2, AXES)),
            pltpu.SemaphoreType.DMA((devices,)),
            pltpu.SemaphoreType.DMA((devices,)),
            pltpu.SemaphoreType.DMA((AXES, CHUNKS)),
        ],
        compiler_params=pltpu.CompilerParams(has_side_effects=True, vmem_limit_bytes=60 * 1024 * 1024),
        name='reduce',
    )(local_grads)
    return g, scale


def update_gather_kernel(grad, master, first, second, scale, rate, working, new_master, new_first, new_second,
                         in_buf, out_buf, in_sem, out_sem, own_ssem, own_rsem, fwd_ssem, fwd_rsem, pair_ssem, pair_rsem):
    me = lax.axis_index('dp')
    partner = bit_flip(me, 1)
    rows, width = grad.shape
    third = width // AXES
    total_rows = working.shape[0]
    pieces = rows // PIECE_ROWS
    inputs = (grad, master, first, second)
    outputs = (new_master, new_first, new_second)

    def piece_at(owner, i, cols):
        return working.at[pl.ds(pl.multiple_of(owner * rows + i * PIECE_ROWS, PIECE_ROWS), PIECE_ROWS), cols]

    def send(owner, i, cols, ssem, rsem, target):
        ref = piece_at(owner, i, cols)
        return pltpu.make_async_remote_copy(src_ref=ref, dst_ref=ref, send_sem=ssem, recv_sem=rsem,
                                            device_id=(target,), device_id_type=MESH)

    every = pl.ds(0, width)

    def cols_of(k):
        return pl.ds((k % AXES) * third, third)

    def chip_flip(*axes):
        mask = 0
        for axis in axes:
            mask ^= 2 << (axis % AXES)
        return bit_flip(me, mask)

    def load(i, n):
        return pltpu.make_async_copy(inputs[n].at[pl.ds(pl.multiple_of(i * PIECE_ROWS, PIECE_ROWS), PIECE_ROWS)], in_buf.at[i % 2, n], in_sem.at[i % 2, n])

    def store(i, n):
        return pltpu.make_async_copy(out_buf.at[i % 2, n], outputs[n].at[pl.ds(pl.multiple_of(i * PIECE_ROWS, PIECE_ROWS), PIECE_ROWS)], out_sem.at[i % 2, n])

    def own_send(i, axis):
        return send(me, i, every, own_ssem.at[axis, i], own_rsem.at[axis, i], chip_flip(axis))

    def own_recv(i, axis):
        return send(chip_flip(axis), i, every, own_ssem.at[axis, i], own_rsem.at[axis, i], chip_flip(axis))

    hops = (((0,), 1), ((0,), 2), ((1,), 2), ((0, 1), 2))

    def fwd_send(i, kind, k):
        source, axis = hops[kind]
        return send(chip_flip(*[k + a for a in source]), i, cols_of(k), fwd_ssem.at[kind, k, i], fwd_rsem.at[kind, k, i], chip_flip(k + axis))

    def fwd_recv(i, kind, k):
        source, axis = hops[kind]
        return send(chip_flip(*[k + a for a in source], k + axis), i, cols_of(k), fwd_ssem.at[kind, k, i], fwd_rsem.at[kind, k, i], chip_flip(k + axis))

    def pair_own(i, parity=0):
        owner = me if parity == 0 else partner
        return send(owner, i, every, pair_ssem.at[0, i], pair_rsem.at[0, i], partner)

    def pair_axis(i, axis, parity=0):
        owner = chip_flip(axis)
        owner = owner if parity == 0 else bit_flip(owner, 1)
        return send(owner, i, every, pair_ssem.at[1 + axis, i], pair_rsem.at[1 + axis, i], partner)

    def pair_fwd(i, kind, k, parity=0):
        source, axis = hops[kind]
        owner = chip_flip(*[k + a for a in source], k + axis)
        owner = owner if parity == 0 else bit_flip(owner, 1)
        slot = 4 + kind * AXES + k
        return send(owner, i, cols_of(k), pair_ssem.at[slot, i], pair_rsem.at[slot, i], partner)

    clip = scale[0, 0]
    learn_rate = rate[0]
    run_starts, lr_values, decay_values = layout_runs(width, total_rows)
    first_norm = 1.0 / (1.0 - 0.9 ** ADAM_STEP)
    second_norm = 1.0 / (1.0 - 0.99 ** ADAM_STEP)

    for n in range(4):
        load(0, n).start()

    def own_piece(i, carry):
        @pl.when(i + 1 < pieces)
        def _():
            for n in range(4):
                load(i + 1, n).start()
        for n in range(4):
            load(i, n).wait()

        @pl.when(i >= 2)
        def _():
            for n in range(3):
                store(i - 2, n).wait()
        slot = i % 2
        group = 16

        def group_step(r, carry):
            lo = pl.multiple_of(r * group, group)
            here = pl.ds(lo, group)
            start = me * rows + i * PIECE_ROWS + lo
            row_ids = start + lax.broadcasted_iota(jnp.int32, (group, 128), 0)
            factor = jnp.full((group, 128), lr_values[0], jnp.float32)
            decay = jnp.full((group, 128), decay_values[0], jnp.float32)
            for r_start, r_lr, r_decay in zip(run_starts[1:], lr_values[1:], decay_values[1:]):
                past = row_ids >= r_start
                factor = jnp.where(past, r_lr, factor)
                decay = jnp.where(past, r_decay, decay)
            step_size = learn_rate * factor
            for tile in range(width // 128):
                at = pl.ds(tile * 128, 128)
                clipped = in_buf[slot, 0, here, at] * clip
                weights = in_buf[slot, 1, here, at]
                moment = 0.9 * in_buf[slot, 2, here, at] + 0.1 * clipped
                square = 0.99 * in_buf[slot, 3, here, at] + 0.01 * (clipped * clipped)
                moved = weights - step_size * ((moment * first_norm) / (jnp.sqrt(square * second_norm) + 1e-8) + decay * weights)
                out_buf[slot, 0, here, at] = moved
                out_buf[slot, 1, here, at] = moment
                out_buf[slot, 2, here, at] = square
                working[pl.ds(pl.multiple_of(start, group), group), at] = moved.astype(jnp.bfloat16)
            return carry

        lax.fori_loop(0, PIECE_ROWS // group, group_step, 0)
        for axis in range(AXES):
            own_send(i, axis).start()
        pair_own(i).start()
        for n in range(3):
            store(i, n).start()
        return carry

    def neighbour_piece(i, carry):
        for axis in range(AXES):
            own_recv(i, axis).wait_recv()
            pair_axis(i, axis).start()
        for kind in range(3):
            for k in range(AXES):
                fwd_send(i, kind, k).start()
        return carry

    def far_piece(i, carry):
        for k in range(AXES):
            fwd_recv(i, 0, k).wait_recv()
            fwd_send(i, 3, k).start()
            pair_fwd(i, 0, k).start()
        for kind in (1, 2):
            for k in range(AXES):
                fwd_recv(i, kind, k).wait_recv()
                pair_fwd(i, kind, k).start()
        return carry

    def last_piece(i, carry):
        for k in range(AXES):
            fwd_recv(i, 3, k).wait_recv()
            pair_fwd(i, 3, k).start()
        return carry

    def drain(i, carry):
        for axis in range(AXES):
            own_send(i, axis).wait_send()
            pair_axis(i, axis).wait_send()
            pair_axis(i, axis, 1).wait_recv()
        pair_own(i).wait_send()
        pair_own(i, 1).wait_recv()
        for kind in range(4):
            for k in range(AXES):
                fwd_send(i, kind, k).wait_send()
                pair_fwd(i, kind, k).wait_send()
                pair_fwd(i, kind, k, 1).wait_recv()
        return carry

    lax.fori_loop(0, pieces, own_piece, 0)
    lax.fori_loop(0, pieces, neighbour_piece, 0)
    for i in (pieces - 2, pieces - 1):
        for n in range(3):
            store(i, n).wait()
    lax.fori_loop(0, pieces, far_piece, 0)
    lax.fori_loop(0, pieces, last_piece, 0)
    lax.fori_loop(0, pieces, drain, 0)


def write_kernel(working, new_master, new_first, new_second, working_out, master_out, first_out, second_out,
                 buf, working_sem, in_sem, out_sem):
    pairs = ((new_master, master_out), (new_first, first_out), (new_second, second_out))
    slots = buf.shape[0]
    piece = buf.shape[1]
    per = master_out.shape[0] // piece
    steps = 3 * per

    def load(s):
        return pltpu.make_async_copy(pairs[s // per][0].at[pl.ds(s % per * piece, piece)], buf.at[s % slots], in_sem.at[s % slots])

    def store(s):
        return pltpu.make_async_copy(buf.at[s % slots], pairs[s // per][1].at[pl.ds(s % per * piece, piece)], out_sem.at[s % slots])

    stripes = working_sem.shape[0]
    stripe = working.shape[0] // stripes

    def put(n):
        here = pl.ds(n * stripe, stripe)
        return pltpu.make_async_copy(working.at[here], working_out.at[here], working_sem.at[n])

    for s in range(slots):
        load(s).start()
    for n in range(stripes):
        put(n).start()
    for s in range(steps):
        load(s).wait()
        store(s).start()
        if s + 1 >= slots and s + 1 < steps:
            store(s + 1 - slots).wait()
            load(s + 1).start()
    for s in range(max(steps - slots, 0), steps):
        store(s).wait()
    for n in range(stripes):
        put(n).wait()


def update_gather(grad, master, first, second, scale, rate, devices):
    rows, width = grad.shape
    any_spec = pl.BlockSpec(memory_space=pltpu.HBM)
    vmem_spec = pl.BlockSpec(memory_space=pltpu.VMEM)
    f32, bf16 = jnp.float32, jnp.bfloat16
    pieces = rows // PIECE_ROWS
    shard = pltpu.HBM((rows, width), f32)
    dma = pltpu.SemaphoreType.DMA
    working, *news = pl.pallas_call(
        update_gather_kernel,
        out_shape=(pltpu.VMEM((devices * rows, width), bf16), shard, shard, shard),
        in_specs=[any_spec] * 4 + [vmem_spec, pl.BlockSpec(memory_space=pltpu.SMEM)],
        out_specs=(vmem_spec, any_spec, any_spec, any_spec),
        scratch_shapes=[
            pltpu.VMEM((2, 4, PIECE_ROWS, width), f32),
            pltpu.VMEM((2, 3, PIECE_ROWS, width), f32),
            dma((2, 4)),
            dma((2, 3)),
            dma((AXES, pieces)),
            dma((AXES, pieces)),
            dma((4, AXES, pieces)),
            dma((4, AXES, pieces)),
            dma((16, pieces)),
            dma((16, pieces)),
        ],
        compiler_params=pltpu.CompilerParams(has_side_effects=True, vmem_limit_bytes=12 * 1024 * 1024),
        name='gather',
    )(grad, master, first, second, scale, rate.reshape(1))
    working_shape = pltpu.HBM((devices * rows, width), bf16)
    return pl.pallas_call(
        write_kernel,
        out_shape=(working_shape, shard, shard, shard),
        in_specs=[vmem_spec, any_spec, any_spec, any_spec],
        out_specs=(any_spec,) * 4,
        scratch_shapes=[pltpu.VMEM((6, rows // 4, width), f32), dma((16,)), dma((6,)), dma((6,))],
        compiler_params=pltpu.CompilerParams(vmem_limit_bytes=12 * 1024 * 1024),
        name='write',
    )(pltpu.with_memory_space_constraint(working, pltpu.VMEM), *news)


def solution(mesh):
    dev_count = mesh.shape['dp']

    def device_step(local_grads, master, mom_first, mom_second, learn_rate):
        grad_shard, clip_scale = reduce_scatter(local_grads, dev_count)
        working, new_master, new_first, new_second = update_gather(grad_shard, master, mom_first, mom_second, clip_scale, learn_rate, dev_count)
        return new_master, new_first, new_second, working

    return jax.shard_map(device_step, mesh=mesh, in_specs=(P('dp', None, None), P('dp', None), P('dp', None), P('dp', None), P()), out_specs=(P('dp', None), P('dp', None), P('dp', None), P(None, None)), check_vma=False)
```

```python
import functools

import jax
import jax.numpy as jnp
from jax import lax
from jax.experimental import pallas as pl
from jax.experimental.pallas import tpu as pltpu
from jax.sharding import PartitionSpec as P

LAYERS = 2
MIX_RANK = 32
DECAY_RANK = 64
ADAM_STEP = 10

AXES = 3
CHUNKS = 4
SLOTS = 3
AHEAD = 4
PIECE_ROWS = 256
LOAD_ROWS = 64
LOADS = 3
MESH = pl.DeviceIdType.MESH


def layout_runs(model_width, total_rows):
    ffn_width = 7 * model_width // 2
    layer_rows = 6 * model_width + 2 * ffn_width + 16 + 10 * MIX_RANK + 2 * DECAY_RANK
    vocab_rows = (total_rows - LAYERS * layer_rows - 4) // 2
    base_rule = (1.0, 0.0)
    decay_rule = (1.0, 0.1)
    time_rule = (2.0, 0.0)
    pieces = [(vocab_rows, decay_rule)]
    for layer_idx in range(LAYERS):
        lead_rows = 12 if layer_idx == 0 else 10
        pieces = pieces + [(lead_rows + 10 * MIX_RANK, base_rule), (1, time_rule), (2 * DECAY_RANK, base_rule), (1, time_rule), (5 * model_width, decay_rule), (4, base_rule), (2 * ffn_width + model_width, decay_rule)]
    pieces = pieces + [(2, base_rule), (vocab_rows, decay_rule)]
    run_starts = []
    next_row = 0
    for run_len, run_rule in pieces:
        run_starts.append(next_row)
        next_row = next_row + run_len
    lr_values = [run_rule[0] for run_len, run_rule in pieces]
    decay_values = [run_rule[1] for run_len, run_rule in pieces]
    return run_starts, lr_values, decay_values


def bit_flip(index, mask):
    flipped = index
    for bit in range(4):
        step = 1 << bit
        if mask & step:
            flipped = flipped + step - 2 * step * ((index // step) % 2)
    return flipped


def reduce_kernel(grads, g_out, c_out, pairs, landed, stage, own_buf, pair_buf, part_buf, norm_buf,
                  pair_ssem, pair_rsem, send_sem, recv_sem, own_sem, pairl_sem, norm_ssem, norm_rsem, g_sem):
    me = lax.axis_index('dp')
    chip, core = me // 2, me % 2
    partner = bit_flip(me, 1)
    rows = g_out.shape[0]
    third = g_out.shape[1] // AXES
    part_rows = rows // CHUNKS
    devices = norm_buf.shape[0]

    def unit_row(j, k, parity):
        flip = chip
        e = 7 - j
        for place in range(AXES):
            step = 1 << ((k + place) % AXES)
            want = (e // (1 << (2 - place))) % 2
            bit = (chip // step) % 2
            flip = flip + want * (step - 2 * step * bit)
        return (2 * flip + parity) * rows

    def pair_copy(s, k):
        j, i = s // CHUNKS, s % CHUNKS
        row = pl.multiple_of(unit_row(j, k, 1 - core) + i * part_rows, part_rows)
        return pltpu.make_async_remote_copy(
            src_ref=grads.at[0, pl.ds(row, part_rows), pl.ds(k * third, third)],
            dst_ref=pairs.at[j, k, pl.ds(pl.multiple_of(i * part_rows, part_rows), part_rows)],
            send_sem=pair_ssem.at[j, k, i],
            recv_sem=pair_rsem.at[j, k, i],
            device_id=(partner,),
            device_id_type=MESH)

    def own_load(s, k):
        j, i = s // CHUNKS, s % CHUNKS
        row = pl.multiple_of(unit_row(j, k, core) + i * part_rows, part_rows)
        return pltpu.make_async_copy(
            grads.at[0, pl.ds(row, part_rows), pl.ds(k * third, third)], own_buf.at[s % 2, k], own_sem.at[s % 2, k])

    def pair_load(s, k):
        j, i = s // CHUNKS, s % CHUNKS
        return pltpu.make_async_copy(
            pairs.at[j, k, pl.ds(pl.multiple_of(i * part_rows, part_rows), part_rows)], pair_buf.at[s % 2, k], pairl_sem.at[s % 2, k])

    def piece_copy(j, i, k, slot, axis):
        return pltpu.make_async_remote_copy(
            src_ref=stage.at[k, slot],
            dst_ref=landed.at[j, k, pl.ds(pl.multiple_of(i * part_rows, part_rows), part_rows)],
            send_sem=send_sem.at[k, slot],
            recv_sem=recv_sem.at[j, k, i],
            device_id=(bit_flip(me, 2 << axis),),
            device_id_type=MESH)

    total_steps = 8 * CHUNKS

    def start_pairs(s):
        for k in range(AXES):
            pair_copy(s, k).start()

    def start_own(s):
        for k in range(AXES):
            own_load(s, k).start()

    def start_pair_loads(s):
        for k in range(AXES):
            pair_copy(s, k).wait_recv()
            pair_load(s, k).start()

    barrier = pltpu.get_barrier_semaphore()
    for d in range(1, devices):
        pl.semaphore_signal(barrier, inc=1, device_id=((me + d) % devices,), device_id_type=MESH)
    start_own(0)
    pl.semaphore_wait(barrier, devices - 1)
    for s in range(AHEAD):
        start_pairs(s)
    start_pair_loads(0)

    def step(s, phase):
        j, i = s // CHUNKS, s % CHUNKS

        @pl.when(s + AHEAD < total_steps)
        def _():
            start_pairs(s + AHEAD)

        @pl.when(s + 1 < total_steps)
        def _():
            start_own(s + 1)

        def load_next():
            @pl.when(s + 1 < total_steps)
            def _():
                start_pair_loads(s + 1)

        if phase == 1:
            sources = []
        elif phase == 2:
            sources = [j - 4]
        elif phase == 3:
            sources = [2, 4]
        else:
            sources = [3, 5, 6]
        slot = s % SLOTS
        base = pl.multiple_of(i * part_rows, part_rows)
        for k in range(AXES):
            own_load(s, k).wait()
            pair_load(s, k).wait()
            for source in sources:
                piece_copy(source, i, k, 0, 0).wait_recv()
            if phase < 4:
                @pl.when(s >= SLOTS)
                def _():
                    piece_copy(0, 0, k, slot, 0).wait_send()
            group = 64

            def add_rows(r, carry):
                lo = pl.multiple_of(r * group, group)
                value = own_buf[s % 2, k, pl.ds(lo, group)].astype(jnp.float32) + pair_buf[s % 2, k, pl.ds(lo, group)].astype(jnp.float32)
                for source in sources:
                    value = value + landed[source, k, pl.ds(base + lo, group)]
                if phase < 4:
                    stage[k, slot, pl.ds(lo, group)] = value
                    return carry
                value = value * (1.0 / devices)
                landed[0, k, pl.ds(base + lo, group)] = value
                return carry + jnp.sum((value * value).reshape(group // 8, 8, third), axis=0)

            if phase < 4:
                lax.fori_loop(0, part_rows // group, add_rows, 0)
            else:
                part_buf[...] += lax.fori_loop(0, part_rows // group, add_rows, jnp.zeros((8, third), jnp.float32))
            if phase < 4:
                piece_copy(j, i, k, slot, (k + phase - 1) % AXES).start()
            else:
                pltpu.make_async_copy(
                    landed.at[0, k, pl.ds(base, part_rows)],
                    g_out.at[pl.ds(base, part_rows), pl.ds(k * third, third)], g_sem.at[k, i]).start()
        load_next()

    part_buf[...] = jnp.zeros_like(part_buf)
    for phase, lo, hi in ((1, 0, 4), (2, 4, 6), (3, 6, 7), (4, 7, 8)):
        def run(s, carry, phase=phase):
            step(s, phase)
            return carry
        lax.fori_loop(lo * CHUNKS, hi * CHUNKS, run, 0)

    part_buf[:, :128] = part_buf[:, :128] + part_buf[:, 128:]
    norm_buf[me] = part_buf[:, :128]

    def norm_copy(d):
        return pltpu.make_async_remote_copy(
            src_ref=part_buf.at[:, pl.ds(0, 128)],
            dst_ref=norm_buf.at[me],
            send_sem=norm_ssem.at[d],
            recv_sem=norm_rsem.at[me],
            device_id=((me + d) % devices,),
            device_id_type=MESH)

    def norm_recv(d):
        sender = (me + devices - d) % devices
        return pltpu.make_async_remote_copy(
            src_ref=part_buf.at[:, pl.ds(0, 128)],
            dst_ref=norm_buf.at[sender],
            send_sem=norm_ssem.at[d],
            recv_sem=norm_rsem.at[sender],
            device_id=(partner,),
            device_id_type=MESH)

    for d in range(1, devices):
        norm_copy(d).start()
    for last in range(SLOTS):
        for k in range(AXES):
            piece_copy(0, 0, k, last, 0).wait_send()
    def drain_pair(s, carry):
        for k in range(AXES):
            pair_copy(s, k).wait_send()
        return carry

    lax.fori_loop(0, total_steps, drain_pair, 0)
    for i in range(CHUNKS):
        for k in range(AXES):
            pltpu.make_async_copy(
                landed.at[0, k, pl.ds(i * part_rows, part_rows)],
                g_out.at[pl.ds(i * part_rows, part_rows), pl.ds(k * third, third)], g_sem.at[k, i]).wait()
    for d in range(1, devices):
        norm_copy(d).wait_send()
    for d in range(1, devices):
        norm_recv(d).wait_recv()
    square_sum = jnp.sum(jnp.sum(norm_buf[...], axis=0), keepdims=True)
    c_out[...] = jnp.broadcast_to(jnp.minimum(1.0, 1.0 / (jnp.sqrt(square_sum) + 1e-6)), c_out.shape)


def reduce_scatter(local_grads, devices):
    total_rows, width = local_grads.shape[1:]
    rows, third = total_rows // devices, width // AXES
    any_spec = pl.BlockSpec(memory_space=pl.ANY)
    f32, bf16 = jnp.float32, jnp.bfloat16
    part_rows = rows // CHUNKS
    g, scale, _ = pl.pallas_call(
        reduce_kernel,
        out_shape=(jax.ShapeDtypeStruct((rows, width), f32),
                   jax.ShapeDtypeStruct((8, 128), f32),
                   jax.ShapeDtypeStruct((8, AXES, rows, third), bf16)),
        in_specs=[any_spec],
        out_specs=(any_spec, pl.BlockSpec(memory_space=pltpu.VMEM), any_spec),
        scratch_shapes=[
            pltpu.VMEM((7, AXES, rows, third), f32),
            pltpu.VMEM((AXES, SLOTS, part_rows, third), f32),
            pltpu.VMEM((2, AXES, part_rows, third), bf16),
            pltpu.VMEM((2, AXES, part_rows, third), bf16),
            pltpu.VMEM((8, third), f32),
            pltpu.VMEM((devices, 8, 128), f32),
            pltpu.SemaphoreType.DMA((8, AXES, CHUNKS)),
            pltpu.SemaphoreType.DMA((8, AXES, CHUNKS)),
            pltpu.SemaphoreType.DMA((AXES, SLOTS)),
            pltpu.SemaphoreType.DMA((7, AXES, CHUNKS)),
            pltpu.SemaphoreType.DMA((2, AXES)),
            pltpu.SemaphoreType.DMA((2, AXES)),
            pltpu.SemaphoreType.DMA((devices,)),
            pltpu.SemaphoreType.DMA((devices,)),
            pltpu.SemaphoreType.DMA((AXES, CHUNKS)),
        ],
        compiler_params=pltpu.CompilerParams(has_side_effects=True, vmem_limit_bytes=60 * 1024 * 1024, collective_id=0),
        name='reduce',
    )(local_grads)
    return g, scale


def update_gather_kernel(grad, master, first, second, scale, rate, working, new_master, new_first, new_second,
                         in_buf, out_buf, in_sem, out_sem, own_ssem, own_rsem, fwd_ssem, fwd_rsem, pair_ssem, pair_rsem):
    me = lax.axis_index('dp')
    partner = bit_flip(me, 1)
    rows, width = grad.shape
    third = width // AXES
    total_rows = working.shape[0]
    pieces = rows // PIECE_ROWS
    inputs = (grad, master, first, second)

    def piece_at(owner, i, cols):
        return working.at[pl.ds(pl.multiple_of(owner * rows + i * PIECE_ROWS, PIECE_ROWS), PIECE_ROWS), cols]

    def send(owner, i, cols, ssem, rsem, target):
        ref = piece_at(owner, i, cols)
        return pltpu.make_async_remote_copy(src_ref=ref, dst_ref=ref, send_sem=ssem, recv_sem=rsem,
                                            device_id=(target,), device_id_type=MESH)

    every = pl.ds(0, width)

    def cols_of(k):
        return pl.ds((k % AXES) * third, third)

    def chip_flip(*axes):
        mask = 0
        for axis in axes:
            mask ^= 2 << (axis % AXES)
        return bit_flip(me, mask)

    def load(t, n):
        here = pl.ds(pl.multiple_of(t * LOAD_ROWS, LOAD_ROWS), LOAD_ROWS)
        return pltpu.make_async_copy(inputs[n].at[here], in_buf.at[t % LOADS, n], in_sem.at[t % LOADS, n])

    def store(t):
        here = pl.ds(pl.multiple_of(t * LOAD_ROWS, LOAD_ROWS), LOAD_ROWS)
        return pltpu.make_async_copy(out_buf.at[t % 2], new_second.at[here], out_sem.at[t % 2])

    def own_send(i, axis):
        return send(me, i, every, own_ssem.at[axis, i], own_rsem.at[axis, i], chip_flip(axis))

    def own_recv(i, axis):
        return send(chip_flip(axis), i, every, own_ssem.at[axis, i], own_rsem.at[axis, i], chip_flip(axis))

    hops = (((0,), 1), ((0,), 2), ((1,), 2), ((0, 1), 2))

    def fwd_send(i, kind, k):
        source, axis = hops[kind]
        return send(chip_flip(*[k + a for a in source]), i, cols_of(k), fwd_ssem.at[kind, k, i], fwd_rsem.at[kind, k, i], chip_flip(k + axis))

    def fwd_recv(i, kind, k):
        source, axis = hops[kind]
        return send(chip_flip(*[k + a for a in source], k + axis), i, cols_of(k), fwd_ssem.at[kind, k, i], fwd_rsem.at[kind, k, i], chip_flip(k + axis))

    def pair_own(i, parity=0):
        owner = me if parity == 0 else partner
        return send(owner, i, every, pair_ssem.at[0, i], pair_rsem.at[0, i], partner)

    def pair_axis(i, axis, parity=0):
        owner = chip_flip(axis)
        owner = owner if parity == 0 else bit_flip(owner, 1)
        return send(owner, i, every, pair_ssem.at[1 + axis, i], pair_rsem.at[1 + axis, i], partner)

    def pair_fwd(i, kind, k, parity=0):
        source, axis = hops[kind]
        owner = chip_flip(*[k + a for a in source], k + axis)
        owner = owner if parity == 0 else bit_flip(owner, 1)
        slot = 4 + kind * AXES + k
        return send(owner, i, cols_of(k), pair_ssem.at[slot, i], pair_rsem.at[slot, i], partner)

    clip = scale[0, 0]
    learn_rate = rate[0]
    run_starts, lr_values, decay_values = layout_runs(width, total_rows)
    first_norm = 1.0 / (1.0 - 0.9 ** ADAM_STEP)
    second_norm = 1.0 / (1.0 - 0.99 ** ADAM_STEP)

    steps = rows // LOAD_ROWS
    barrier = pltpu.get_barrier_semaphore()
    peers = [partner] + [chip_flip(axis) for axis in range(AXES)]
    for peer in peers:
        pl.semaphore_signal(barrier, inc=1, device_id=(peer,), device_id_type=MESH)
    for t in range(LOADS):
        for n in range(4):
            load(t, n).start()
    pl.semaphore_wait(barrier, len(peers))

    def update_rows(t, carry):
        for n in range(4):
            load(t, n).wait()

        @pl.when(t >= 2)
        def _():
            store(t - 2).wait()
        slot = t % LOADS
        out_slot = t % 2
        group = 16

        def group_step(r, carry):
            lo = pl.multiple_of(r * group, group)
            here = pl.ds(lo, group)
            row = pl.multiple_of(t * LOAD_ROWS + lo, group)
            start = me * rows + row
            row_ids = start + lax.broadcasted_iota(jnp.int32, (group, 128), 0)
            factor = jnp.full((group, 128), lr_values[0], jnp.float32)
            decay = jnp.full((group, 128), decay_values[0], jnp.float32)
            for r_start, r_lr, r_decay in zip(run_starts[1:], lr_values[1:], decay_values[1:]):
                past = row_ids >= r_start
                factor = jnp.where(past, r_lr, factor)
                decay = jnp.where(past, r_decay, decay)
            step_size = learn_rate * factor
            for tile in range(width // 128):
                at = pl.ds(tile * 128, 128)
                clipped = in_buf[slot, 0, here, at] * clip
                weights = in_buf[slot, 1, here, at]
                moment = 0.9 * in_buf[slot, 2, here, at] + 0.1 * clipped
                square = 0.99 * in_buf[slot, 3, here, at] + 0.01 * (clipped * clipped)
                moved = weights - step_size * ((moment * first_norm) / (jnp.sqrt(square * second_norm) + 1e-8) + decay * weights)
                new_master[pl.ds(row, group), at] = moved
                new_first[pl.ds(row, group), at] = moment
                out_buf[out_slot, here, at] = square
                working[pl.ds(pl.multiple_of(start, group), group), at] = moved.astype(jnp.bfloat16)
            return carry

        lax.fori_loop(0, LOAD_ROWS // group, group_step, 0)
        store(t).start()

        @pl.when(t + LOADS < steps)
        def _():
            for n in range(4):
                load(t + LOADS, n).start()
        return carry

    def own_piece(i, carry):
        per = PIECE_ROWS // LOAD_ROWS
        lax.fori_loop(i * per, (i + 1) * per, update_rows, 0)
        for axis in range(AXES):
            own_send(i, axis).start()
        pair_own(i).start()
        return carry

    def neighbour_piece(i, carry):
        for axis in range(AXES):
            own_recv(i, axis).wait_recv()
            pair_axis(i, axis).start()
        for kind in range(3):
            for k in range(AXES):
                fwd_send(i, kind, k).start()
        return carry

    def far_piece(i, carry):
        for k in range(AXES):
            fwd_recv(i, 0, k).wait_recv()
            fwd_send(i, 3, k).start()
            pair_fwd(i, 0, k).start()
        for kind in (1, 2):
            for k in range(AXES):
                fwd_recv(i, kind, k).wait_recv()
                pair_fwd(i, kind, k).start()
        return carry

    def last_piece(i, carry):
        for k in range(AXES):
            fwd_recv(i, 3, k).wait_recv()
            pair_fwd(i, 3, k).start()
        return carry

    def drain(i, carry):
        for axis in range(AXES):
            own_send(i, axis).wait_send()
            pair_axis(i, axis).wait_send()
            pair_axis(i, axis, 1).wait_recv()
        pair_own(i).wait_send()
        pair_own(i, 1).wait_recv()
        for kind in range(4):
            for k in range(AXES):
                fwd_send(i, kind, k).wait_send()
                pair_fwd(i, kind, k).wait_send()
                pair_fwd(i, kind, k, 1).wait_recv()
        return carry

    lax.fori_loop(0, pieces, own_piece, 0)
    lax.fori_loop(0, pieces, neighbour_piece, 0)
    for t in (steps - 2, steps - 1):
        store(t).wait()
    lax.fori_loop(0, pieces, far_piece, 0)
    lax.fori_loop(0, pieces, last_piece, 0)
    lax.fori_loop(0, pieces, drain, 0)


def write_kernel(working, new_master, new_first, new_second, working_out, master_out, first_out, second_out,
                 buf, put_sem, in_sem, out_sem):
    rows = new_second.shape[0]
    slots, piece = buf.shape[:2]
    steps = rows // piece

    def load(s):
        return pltpu.make_async_copy(new_second.at[pl.ds(s * piece, piece)], buf.at[s % slots], in_sem.at[s % slots])

    def store(s):
        return pltpu.make_async_copy(buf.at[s % slots], second_out.at[pl.ds(s * piece, piece)], out_sem.at[s % slots])

    puts = [pltpu.make_async_copy(new_master, master_out, put_sem.at[0]), pltpu.make_async_copy(new_first, first_out, put_sem.at[1])]
    stripes = put_sem.shape[0] - 2
    stripe = working.shape[0] // stripes
    for n in range(stripes):
        here = pl.ds(n * stripe, stripe)
        puts.append(pltpu.make_async_copy(working.at[here], working_out.at[here], put_sem.at[n + 2]))

    for s in range(slots):
        load(s).start()
    for s in range(steps):
        for put in puts[s * len(puts) // steps:(s + 1) * len(puts) // steps]:
            put.start()
        load(s).wait()
        store(s).start()
        if s + 1 >= slots and s + 1 < steps:
            store(s + 1 - slots).wait()
            load(s + 1).start()
    for s in range(steps - slots, steps):
        store(s).wait()
    for put in puts:
        put.wait()


def update_gather(grad, master, first, second, scale, rate, devices):
    rows, width = grad.shape
    any_spec = pl.BlockSpec(memory_space=pltpu.HBM)
    vmem_spec = pl.BlockSpec(memory_space=pltpu.VMEM)
    f32, bf16 = jnp.float32, jnp.bfloat16
    pieces = rows // PIECE_ROWS
    shard = pltpu.HBM((rows, width), f32)
    near = pltpu.VMEM((rows, width), f32)
    dma = pltpu.SemaphoreType.DMA
    working, new_master, new_first, new_second = pl.pallas_call(
        update_gather_kernel,
        out_shape=(pltpu.VMEM((devices * rows, width), bf16), near, near, shard),
        in_specs=[any_spec] * 4 + [vmem_spec, pl.BlockSpec(memory_space=pltpu.SMEM)],
        out_specs=(vmem_spec, vmem_spec, vmem_spec, any_spec),
        scratch_shapes=[
            pltpu.VMEM((LOADS, 4, LOAD_ROWS, width), f32),
            pltpu.VMEM((2, LOAD_ROWS, width), f32),
            dma((LOADS, 4)),
            dma((2,)),
            dma((AXES, pieces)),
            dma((AXES, pieces)),
            dma((4, AXES, pieces)),
            dma((4, AXES, pieces)),
            dma((16, pieces)),
            dma((16, pieces)),
        ],
        compiler_params=pltpu.CompilerParams(has_side_effects=True, vmem_limit_bytes=3 * 1024 * 1024, collective_id=1),
        name='gather',
    )(grad, master, first, second, scale, rate.reshape(1))
    working_shape = pltpu.HBM((devices * rows, width), bf16)
    return pl.pallas_call(
        write_kernel,
        out_shape=(working_shape, shard, shard, shard),
        in_specs=[vmem_spec, vmem_spec, vmem_spec, any_spec],
        out_specs=(any_spec,) * 4,
        scratch_shapes=[pltpu.VMEM((3, rows // 8, width), f32), dma((18,)), dma((3,)), dma((3,))],
        compiler_params=pltpu.CompilerParams(vmem_limit_bytes=3 * 1024 * 1024),
        name='write',
    )(*[pltpu.with_memory_space_constraint(x, pltpu.VMEM) for x in (working, new_master, new_first)], new_second)


def solution(mesh):
    dev_count = mesh.shape['dp']

    def device_step(local_grads, master, mom_first, mom_second, learn_rate):
        grad_shard, clip_scale = reduce_scatter(local_grads, dev_count)
        working, new_master, new_first, new_second = update_gather(grad_shard, master, mom_first, mom_second, clip_scale, learn_rate, dev_count)
        return new_master, new_first, new_second, working

    return jax.shard_map(device_step, mesh=mesh, in_specs=(P('dp', None, None), P('dp', None), P('dp', None), P('dp', None), P()), out_specs=(P('dp', None), P('dp', None), P('dp', None), P(None, None)), check_vma=False)
```

```python
import functools

import jax
import jax.numpy as jnp
from jax import lax
from jax.experimental import pallas as pl
from jax.experimental.pallas import tpu as pltpu
from jax.sharding import PartitionSpec as P

LAYERS = 2
MIX_RANK = 32
DECAY_RANK = 64
ADAM_STEP = 10

AXES = 3
UNITS = 7
CHUNKS = 4
SLOTS = 3
AHEAD = 4
PIECE_ROWS = 256
FORWARD_ROWS = (512, 512, 512, 512)
LOAD_ROWS = 64
LOADS = 3
MESH = pl.DeviceIdType.MESH


def layout_runs(model_width, total_rows):
    ffn_width = 7 * model_width // 2
    layer_rows = 6 * model_width + 2 * ffn_width + 16 + 10 * MIX_RANK + 2 * DECAY_RANK
    vocab_rows = (total_rows - LAYERS * layer_rows - 4) // 2
    base_rule = (1.0, 0.0)
    decay_rule = (1.0, 0.1)
    time_rule = (2.0, 0.0)
    pieces = [(vocab_rows, decay_rule)]
    for layer_idx in range(LAYERS):
        lead_rows = 12 if layer_idx == 0 else 10
        pieces = pieces + [(lead_rows + 10 * MIX_RANK, base_rule), (1, time_rule), (2 * DECAY_RANK, base_rule), (1, time_rule), (5 * model_width, decay_rule), (4, base_rule), (2 * ffn_width + model_width, decay_rule)]
    pieces = pieces + [(2, base_rule), (vocab_rows, decay_rule)]
    run_starts = []
    next_row = 0
    for run_len, run_rule in pieces:
        run_starts.append(next_row)
        next_row = next_row + run_len
    lr_values = [run_rule[0] for run_len, run_rule in pieces]
    decay_values = [run_rule[1] for run_len, run_rule in pieces]
    return run_starts, lr_values, decay_values


def bit_flip(index, mask):
    flipped = index
    for bit in range(4):
        step = 1 << bit
        if mask & step:
            flipped = flipped + step - 2 * step * ((index // step) % 2)
    return flipped


def reduce_kernel(grads, g_out, c_out, pairs, landed, raw, stage, own_buf, pair_buf, part_buf, norm_buf,
                  pair_ssem, pair_rsem, send_sem, recv_sem, own_sem, pairl_sem, raw_ssem, raw_rsem, norm_ssem, norm_rsem, g_sem):
    me = lax.axis_index('dp')
    chip, core = me // 2, me % 2
    partner = bit_flip(me, 1)
    rows = g_out.shape[0]
    third = g_out.shape[1] // AXES
    part_rows = rows // CHUNKS
    devices = norm_buf.shape[0]

    def unit_row(j, k, parity):
        flip = chip
        e = 7 - j - (j + 4) // 7
        for place in range(AXES):
            step = 1 << ((k + place) % AXES)
            want = (e // (1 << (2 - place))) % 2
            bit = (chip // step) % 2
            flip = flip + want * (step - 2 * step * bit)
        return (2 * flip + parity) * rows

    def raw_copy(k, parity):
        owner = 2 * (bit_flip(me, 2 << k) // 2) + parity
        return pltpu.make_async_remote_copy(
            src_ref=grads.at[0, pl.ds(pl.multiple_of(owner * rows, rows), rows), pl.ds(k * third, third)],
            dst_ref=raw.at[k, core],
            send_sem=raw_ssem.at[k, parity],
            recv_sem=raw_rsem.at[k, core],
            device_id=(owner,),
            device_id_type=MESH)

    def raw_recv(k, parity):
        return pltpu.make_async_remote_copy(
            src_ref=grads.at[0, pl.ds(0, rows), pl.ds(k * third, third)],
            dst_ref=raw.at[k, parity],
            send_sem=raw_ssem.at[k, parity],
            recv_sem=raw_rsem.at[k, parity],
            device_id=(partner,),
            device_id_type=MESH)

    def pair_copy(s, k):
        j, i = s // CHUNKS, s % CHUNKS
        row = pl.multiple_of(unit_row(j, k, 1 - core) + i * part_rows, part_rows)
        return pltpu.make_async_remote_copy(
            src_ref=grads.at[0, pl.ds(row, part_rows), pl.ds(k * third, third)],
            dst_ref=pairs.at[j, k, pl.ds(pl.multiple_of(i * part_rows, part_rows), part_rows)],
            send_sem=pair_ssem.at[j, k, i],
            recv_sem=pair_rsem.at[j, k, i],
            device_id=(partner,),
            device_id_type=MESH)

    def own_load(s, k):
        j, i = s // CHUNKS, s % CHUNKS
        row = pl.multiple_of(unit_row(j, k, core) + i * part_rows, part_rows)
        return pltpu.make_async_copy(
            grads.at[0, pl.ds(row, part_rows), pl.ds(k * third, third)], own_buf.at[s % 2, k], own_sem.at[s % 2, k])

    def pair_load(s, k):
        j, i = s // CHUNKS, s % CHUNKS
        return pltpu.make_async_copy(
            pairs.at[j, k, pl.ds(pl.multiple_of(i * part_rows, part_rows), part_rows)], pair_buf.at[s % 2, k], pairl_sem.at[s % 2, k])

    def piece_copy(j, i, k, slot, axis):
        return pltpu.make_async_remote_copy(
            src_ref=stage.at[k, slot],
            dst_ref=landed.at[j, k, pl.ds(pl.multiple_of(i * part_rows, part_rows), part_rows)],
            send_sem=send_sem.at[k, slot],
            recv_sem=recv_sem.at[j, k, i],
            device_id=(bit_flip(me, 2 << axis),),
            device_id_type=MESH)

    total_steps = UNITS * CHUNKS

    def start_pairs(s):
        for k in range(AXES):
            pair_copy(s, k).start()

    def start_own(s):
        for k in range(AXES):
            own_load(s, k).start()

    def start_pair_loads(s):
        for k in range(AXES):
            pair_copy(s, k).wait_recv()
            pair_load(s, k).start()

    barrier = pltpu.get_barrier_semaphore()
    peers = [partner]
    for k in range(AXES):
        across = 2 * (bit_flip(me, 2 << k) // 2)
        peers += [across, across + 1]
    for peer in peers:
        pl.semaphore_signal(barrier, inc=1, device_id=(peer,), device_id_type=MESH)
    start_own(0)
    pl.semaphore_wait(barrier, len(peers))
    for parity in range(2):
        for k in range(AXES):
            raw_copy(k, parity).start()
    for s in range(AHEAD):
        start_pairs(s)
    start_pair_loads(0)

    def step(s, phase):
        j, i = s // CHUNKS, s % CHUNKS

        @pl.when(s + AHEAD < total_steps)
        def _():
            start_pairs(s + AHEAD)

        @pl.when(s + 1 < total_steps)
        def _():
            start_own(s + 1)

        def load_next():
            @pl.when(s + 1 < total_steps)
            def _():
                start_pair_loads(s + 1)

        if phase == 1:
            sources = []
        elif phase == 2:
            sources = [j - 3]
        elif phase == 3:
            sources = [2, 3]
        else:
            sources = [4, 5]
        slot = s % SLOTS
        base = pl.multiple_of(i * part_rows, part_rows)
        for k in range(AXES):
            own_load(s, k).wait()
            pair_load(s, k).wait()
            for source in sources:
                piece_copy(source, i, k, 0, 0).wait_recv()
            if phase < 4:
                @pl.when(s >= SLOTS)
                def _():
                    piece_copy(0, 0, k, slot, 0).wait_send()
            group = 64

            def add_rows(r, carry):
                lo = pl.multiple_of(r * group, group)
                value = own_buf[s % 2, k, pl.ds(lo, group)].astype(jnp.float32) + pair_buf[s % 2, k, pl.ds(lo, group)].astype(jnp.float32)
                for source in sources:
                    value = value + landed[source, k, pl.ds(base + lo, group)]
                if phase < 4:
                    stage[k, slot, pl.ds(lo, group)] = value
                    return carry
                for parity in range(2):
                    value = value + raw[k, parity, pl.ds(base + lo, group)].astype(jnp.float32)
                value = value * (1.0 / devices)
                landed[0, k, pl.ds(base + lo, group)] = value
                return carry + jnp.sum((value * value).reshape(group // 8, 8, third), axis=0)

            if phase < 4:
                lax.fori_loop(0, part_rows // group, add_rows, 0)
            else:
                part_buf[...] += lax.fori_loop(0, part_rows // group, add_rows, jnp.zeros((8, third), jnp.float32))
            if phase < 4:
                piece_copy(j, i, k, slot, (k + phase - 1) % AXES).start()
            else:
                pltpu.make_async_copy(
                    landed.at[0, k, pl.ds(base, part_rows)],
                    g_out.at[pl.ds(base, part_rows), pl.ds(k * third, third)], g_sem.at[k, i]).start()
        load_next()

    def drain_pair(s, carry):
        for k in range(AXES):
            pair_copy(s, k).wait_send()
        return carry

    part_buf[...] = jnp.zeros_like(part_buf)
    for phase, lo, hi in ((1, 0, 3), (2, 3, 5), (3, 5, 6), (4, 6, 7)):
        def run(s, carry, phase=phase):
            step(s, phase)
            return carry
        if phase == 4:
            lax.fori_loop(0, total_steps, drain_pair, 0)
            for k in range(AXES):
                for parity in range(2):
                    raw_recv(k, parity).wait_recv()
                    raw_copy(k, parity).wait_send()
        lax.fori_loop(lo * CHUNKS, hi * CHUNKS, run, 0)

    part_buf[:, :128] = part_buf[:, :128] + part_buf[:, 128:]
    norm_buf[me] = part_buf[:, :128]

    def norm_copy(d):
        return pltpu.make_async_remote_copy(
            src_ref=part_buf.at[:, pl.ds(0, 128)],
            dst_ref=norm_buf.at[me],
            send_sem=norm_ssem.at[d],
            recv_sem=norm_rsem.at[me],
            device_id=((me + d) % devices,),
            device_id_type=MESH)

    def norm_recv(d):
        sender = (me + devices - d) % devices
        return pltpu.make_async_remote_copy(
            src_ref=part_buf.at[:, pl.ds(0, 128)],
            dst_ref=norm_buf.at[sender],
            send_sem=norm_ssem.at[d],
            recv_sem=norm_rsem.at[sender],
            device_id=(partner,),
            device_id_type=MESH)

    for d in range(1, devices):
        norm_copy(d).start()
    for last in range(SLOTS):
        for k in range(AXES):
            piece_copy(0, 0, k, last, 0).wait_send()
    for i in range(CHUNKS):
        for k in range(AXES):
            pltpu.make_async_copy(
                landed.at[0, k, pl.ds(i * part_rows, part_rows)],
                g_out.at[pl.ds(i * part_rows, part_rows), pl.ds(k * third, third)], g_sem.at[k, i]).wait()
    for d in range(1, devices):
        norm_copy(d).wait_send()
    for d in range(1, devices):
        norm_recv(d).wait_recv()
    square_sum = jnp.sum(jnp.sum(norm_buf[...], axis=0), keepdims=True)
    c_out[...] = jnp.broadcast_to(jnp.minimum(1.0, 1.0 / (jnp.sqrt(square_sum) + 1e-6)), c_out.shape)


def reduce_scatter(local_grads, devices):
    total_rows, width = local_grads.shape[1:]
    rows, third = total_rows // devices, width // AXES
    any_spec = pl.BlockSpec(memory_space=pl.ANY)
    f32, bf16 = jnp.float32, jnp.bfloat16
    part_rows = rows // CHUNKS
    g, scale, _ = pl.pallas_call(
        reduce_kernel,
        out_shape=(jax.ShapeDtypeStruct((rows, width), f32),
                   jax.ShapeDtypeStruct((8, 128), f32),
                   jax.ShapeDtypeStruct((UNITS, AXES, rows, third), bf16)),
        in_specs=[any_spec],
        out_specs=(any_spec, pl.BlockSpec(memory_space=pltpu.VMEM), any_spec),
        scratch_shapes=[
            pltpu.VMEM((UNITS - 1, AXES, rows, third), f32),
            pltpu.VMEM((AXES, 2, rows, third), bf16),
            pltpu.VMEM((AXES, SLOTS, part_rows, third), f32),
            pltpu.VMEM((2, AXES, part_rows, third), bf16),
            pltpu.VMEM((2, AXES, part_rows, third), bf16),
            pltpu.VMEM((8, third), f32),
            pltpu.VMEM((devices, 8, 128), f32),
            pltpu.SemaphoreType.DMA((UNITS, AXES, CHUNKS)),
            pltpu.SemaphoreType.DMA((UNITS, AXES, CHUNKS)),
            pltpu.SemaphoreType.DMA((AXES, SLOTS)),
            pltpu.SemaphoreType.DMA((UNITS - 1, AXES, CHUNKS)),
            pltpu.SemaphoreType.DMA((2, AXES)),
            pltpu.SemaphoreType.DMA((2, AXES)),
            pltpu.SemaphoreType.DMA((AXES, 2)),
            pltpu.SemaphoreType.DMA((AXES, 2)),
            pltpu.SemaphoreType.DMA((devices,)),
            pltpu.SemaphoreType.DMA((devices,)),
            pltpu.SemaphoreType.DMA((AXES, CHUNKS)),
        ],
        compiler_params=pltpu.CompilerParams(has_side_effects=True, vmem_limit_bytes=60 * 1024 * 1024, collective_id=0),
        name='reduce',
    )(local_grads)
    return g, scale


def update_gather_kernel(grad, master, first, second, scale, rate, working, new_master, new_first, new_second,
                         in_buf, out_buf, in_sem, out_sem, own_ssem, own_rsem, fwd_ssem, fwd_rsem, pair_ssem, pair_rsem):
    me = lax.axis_index('dp')
    partner = bit_flip(me, 1)
    rows, width = grad.shape
    third = width // AXES
    total_rows = working.shape[0]
    pieces = rows // PIECE_ROWS
    inputs = (grad, master, first, second)

    def piece_at(owner, i, cols, piece_rows):
        return working.at[pl.ds(pl.multiple_of(owner * rows + i * piece_rows, piece_rows), piece_rows), cols]

    def send(owner, i, cols, ssem, rsem, target, piece_rows=PIECE_ROWS):
        ref = piece_at(owner, i, cols, piece_rows)
        return pltpu.make_async_remote_copy(src_ref=ref, dst_ref=ref, send_sem=ssem, recv_sem=rsem,
                                            device_id=(target,), device_id_type=MESH)

    every = pl.ds(0, width)

    def cols_of(k):
        return pl.ds((k % AXES) * third, third)

    def chip_flip(*axes):
        mask = 0
        for axis in axes:
            mask ^= 2 << (axis % AXES)
        return bit_flip(me, mask)

    def load(t, n):
        here = pl.ds(pl.multiple_of(t * LOAD_ROWS, LOAD_ROWS), LOAD_ROWS)
        return pltpu.make_async_copy(inputs[n].at[here], in_buf.at[t % LOADS, n], in_sem.at[t % LOADS, n])

    def store(t):
        here = pl.ds(pl.multiple_of(t * LOAD_ROWS, LOAD_ROWS), LOAD_ROWS)
        return pltpu.make_async_copy(out_buf.at[t % 2], new_second.at[here], out_sem.at[t % 2])

    def own_send(i, axis):
        return send(me, i, every, own_ssem.at[axis, i], own_rsem.at[axis, i], chip_flip(axis))

    def own_recv(i, axis):
        return send(chip_flip(axis), i, every, own_ssem.at[axis, i], own_rsem.at[axis, i], chip_flip(axis))

    hops = (((0,), 1), ((0,), 2), ((1,), 2), ((0, 1), 2))

    def fwd_send(i, kind, k):
        source, axis = hops[kind]
        return send(chip_flip(*[k + a for a in source]), i, cols_of(k), fwd_ssem.at[kind, k, i], fwd_rsem.at[kind, k, i], chip_flip(k + axis), FORWARD_ROWS[kind])

    def fwd_recv(i, kind, k):
        source, axis = hops[kind]
        return send(chip_flip(*[k + a for a in source], k + axis), i, cols_of(k), fwd_ssem.at[kind, k, i], fwd_rsem.at[kind, k, i], chip_flip(k + axis), FORWARD_ROWS[kind])

    def pair_own(i, parity=0):
        owner = me if parity == 0 else partner
        return send(owner, i, every, pair_ssem.at[0, i], pair_rsem.at[0, i], partner)

    def pair_axis(i, axis, parity=0):
        owner = chip_flip(axis)
        owner = owner if parity == 0 else bit_flip(owner, 1)
        return send(owner, i, every, pair_ssem.at[1 + axis, i], pair_rsem.at[1 + axis, i], partner)

    def pair_fwd(i, kind, k, parity=0):
        source, axis = hops[kind]
        owner = chip_flip(*[k + a for a in source], k + axis)
        owner = owner if parity == 0 else bit_flip(owner, 1)
        slot = 4 + kind * AXES + k
        return send(owner, i, cols_of(k), pair_ssem.at[slot, i], pair_rsem.at[slot, i], partner, FORWARD_ROWS[kind])

    clip = scale[0, 0]
    learn_rate = rate[0]
    run_starts, lr_values, decay_values = layout_runs(width, total_rows)
    first_norm = 1.0 / (1.0 - 0.9 ** ADAM_STEP)
    second_norm = 1.0 / (1.0 - 0.99 ** ADAM_STEP)

    steps = rows // LOAD_ROWS
    barrier = pltpu.get_barrier_semaphore()
    peers = [partner] + [chip_flip(axis) for axis in range(AXES)]
    for peer in peers:
        pl.semaphore_signal(barrier, inc=1, device_id=(peer,), device_id_type=MESH)
    for t in range(LOADS):
        for n in range(4):
            load(t, n).start()
    def update_rows(t, carry):
        for n in range(4):
            load(t, n).wait()

        @pl.when(t >= 2)
        def _():
            store(t - 2).wait()
        slot = t % LOADS
        out_slot = t % 2
        group = 16

        def group_step(r, carry):
            lo = pl.multiple_of(r * group, group)
            here = pl.ds(lo, group)
            row = pl.multiple_of(t * LOAD_ROWS + lo, group)
            start = me * rows + row
            row_ids = start + lax.broadcasted_iota(jnp.int32, (group, 128), 0)
            factor = jnp.full((group, 128), lr_values[0], jnp.float32)
            decay = jnp.full((group, 128), decay_values[0], jnp.float32)
            for r_start, r_lr, r_decay in zip(run_starts[1:], lr_values[1:], decay_values[1:]):
                past = row_ids >= r_start
                factor = jnp.where(past, r_lr, factor)
                decay = jnp.where(past, r_decay, decay)
            step_size = learn_rate * factor
            for tile in range(width // 128):
                at = pl.ds(tile * 128, 128)
                clipped = in_buf[slot, 0, here, at] * clip
                weights = in_buf[slot, 1, here, at]
                moment = 0.9 * in_buf[slot, 2, here, at] + 0.1 * clipped
                square = 0.99 * in_buf[slot, 3, here, at] + 0.01 * (clipped * clipped)
                moved = weights - step_size * ((moment * first_norm) / (jnp.sqrt(square * second_norm) + 1e-8) + decay * weights)
                new_master[pl.ds(row, group), at] = moved
                new_first[pl.ds(row, group), at] = moment
                out_buf[out_slot, here, at] = square
                working[pl.ds(pl.multiple_of(start, group), group), at] = moved.astype(jnp.bfloat16)
            return carry

        lax.fori_loop(0, LOAD_ROWS // group, group_step, 0)
        store(t).start()

        @pl.when(t + LOADS < steps)
        def _():
            for n in range(4):
                load(t + LOADS, n).start()
        return carry

    def own_piece(i, carry):
        per = PIECE_ROWS // LOAD_ROWS
        lax.fori_loop(i * per, (i + 1) * per, update_rows, 0)

        @pl.when(i == 0)
        def _():
            pl.semaphore_wait(barrier, len(peers))
        for axis in range(AXES):
            own_send(i, axis).start()
        pair_own(i).start()
        return carry

    def neighbour_piece(i, carry):
        per = FORWARD_ROWS[0] // PIECE_ROWS
        for part in range(per):
            for axis in range(AXES):
                own_recv(i * per + part, axis).wait_recv()
                pair_axis(i * per + part, axis).start()
        for kind in range(3):
            for k in range(AXES):
                fwd_send(i, kind, k).start()
        return carry

    def far_piece(i, carry):
        per = FORWARD_ROWS[0] // FORWARD_ROWS[3]
        for k in range(AXES):
            fwd_recv(i, 0, k).wait_recv()
            for part in range(per):
                fwd_send(i * per + part, 3, k).start()
            pair_fwd(i, 0, k).start()
        for kind in (1, 2):
            for k in range(AXES):
                fwd_recv(i, kind, k).wait_recv()
                pair_fwd(i, kind, k).start()
        return carry

    def last_piece(i, carry):
        for k in range(AXES):
            fwd_recv(i, 3, k).wait_recv()
            pair_fwd(i, 3, k).start()
        return carry

    def drain_own(i, carry):
        for axis in range(AXES):
            own_send(i, axis).wait_send()
            pair_axis(i, axis).wait_send()
            pair_axis(i, axis, 1).wait_recv()
        pair_own(i).wait_send()
        pair_own(i, 1).wait_recv()
        return carry

    def drain_fwd(i, carry, kinds):
        for kind in kinds:
            for k in range(AXES):
                fwd_send(i, kind, k).wait_send()
                pair_fwd(i, kind, k).wait_send()
                pair_fwd(i, kind, k, 1).wait_recv()
        return carry

    near_pieces, far_pieces = rows // FORWARD_ROWS[0], rows // FORWARD_ROWS[3]
    lax.fori_loop(0, pieces, own_piece, 0)
    lax.fori_loop(0, near_pieces, neighbour_piece, 0)
    for t in (steps - 2, steps - 1):
        store(t).wait()
    lax.fori_loop(0, pieces, drain_own, 0)
    lax.fori_loop(0, near_pieces, far_piece, 0)
    lax.fori_loop(0, near_pieces, functools.partial(drain_fwd, kinds=(0, 1, 2)), 0)
    lax.fori_loop(0, far_pieces, last_piece, 0)
    lax.fori_loop(0, far_pieces, functools.partial(drain_fwd, kinds=(3,)), 0)


def write_kernel(working, new_master, new_first, new_second, working_out, master_out, first_out, second_out,
                 buf, put_sem, in_sem, out_sem):
    rows = new_second.shape[0]
    slots, piece = buf.shape[:2]
    steps = rows // piece

    def load(s):
        return pltpu.make_async_copy(new_second.at[pl.ds(s * piece, piece)], buf.at[s % slots], in_sem.at[s % slots])

    def store(s):
        return pltpu.make_async_copy(buf.at[s % slots], second_out.at[pl.ds(s * piece, piece)], out_sem.at[s % slots])

    puts = [pltpu.make_async_copy(new_master, master_out, put_sem.at[0]), pltpu.make_async_copy(new_first, first_out, put_sem.at[1])]
    stripes = put_sem.shape[0] - 2
    stripe = working.shape[0] // stripes
    for n in range(stripes):
        here = pl.ds(n * stripe, stripe)
        puts.append(pltpu.make_async_copy(working.at[here], working_out.at[here], put_sem.at[n + 2]))

    for s in range(slots):
        load(s).start()
    for s in range(steps):
        for put in puts[s * len(puts) // steps:(s + 1) * len(puts) // steps]:
            put.start()
        load(s).wait()
        store(s).start()
        if s + 1 >= slots and s + 1 < steps:
            store(s + 1 - slots).wait()
            load(s + 1).start()
    for s in range(steps - slots, steps):
        store(s).wait()
    for put in puts:
        put.wait()


def update_gather(grad, master, first, second, scale, rate, devices):
    rows, width = grad.shape
    any_spec = pl.BlockSpec(memory_space=pltpu.HBM)
    vmem_spec = pl.BlockSpec(memory_space=pltpu.VMEM)
    f32, bf16 = jnp.float32, jnp.bfloat16
    pieces = rows // PIECE_ROWS
    shard = pltpu.HBM((rows, width), f32)
    near = pltpu.VMEM((rows, width), f32)
    dma = pltpu.SemaphoreType.DMA
    working, new_master, new_first, new_second = pl.pallas_call(
        update_gather_kernel,
        out_shape=(pltpu.VMEM((devices * rows, width), bf16), near, near, shard),
        in_specs=[any_spec] * 4 + [vmem_spec, pl.BlockSpec(memory_space=pltpu.SMEM)],
        out_specs=(vmem_spec, vmem_spec, vmem_spec, any_spec),
        scratch_shapes=[
            pltpu.VMEM((LOADS, 4, LOAD_ROWS, width), f32),
            pltpu.VMEM((2, LOAD_ROWS, width), f32),
            dma((LOADS, 4)),
            dma((2,)),
            dma((AXES, pieces)),
            dma((AXES, pieces)),
            dma((4, AXES, rows // min(FORWARD_ROWS))),
            dma((4, AXES, rows // min(FORWARD_ROWS))),
            dma((16, rows // min(min(FORWARD_ROWS), PIECE_ROWS))),
            dma((16, rows // min(min(FORWARD_ROWS), PIECE_ROWS))),
        ],
        compiler_params=pltpu.CompilerParams(has_side_effects=True, vmem_limit_bytes=3 * 1024 * 1024, collective_id=1),
        name='gather',
    )(grad, master, first, second, scale, rate.reshape(1))
    working_shape = pltpu.HBM((devices * rows, width), bf16)
    return pl.pallas_call(
        write_kernel,
        out_shape=(working_shape, shard, shard, shard),
        in_specs=[vmem_spec, vmem_spec, vmem_spec, any_spec],
        out_specs=(any_spec,) * 4,
        scratch_shapes=[pltpu.VMEM((3, rows // 8, width), f32), dma((18,)), dma((3,)), dma((3,))],
        compiler_params=pltpu.CompilerParams(vmem_limit_bytes=3 * 1024 * 1024),
        name='write',
    )(*[pltpu.with_memory_space_constraint(x, pltpu.VMEM) for x in (working, new_master, new_first)], new_second)


def solution(mesh):
    dev_count = mesh.shape['dp']

    def device_step(local_grads, master, mom_first, mom_second, learn_rate):
        grad_shard, clip_scale = reduce_scatter(local_grads, dev_count)
        working, new_master, new_first, new_second = update_gather(grad_shard, master, mom_first, mom_second, clip_scale, learn_rate, dev_count)
        return new_master, new_first, new_second, working

    return jax.shard_map(device_step, mesh=mesh, in_specs=(P('dp', None, None), P('dp', None), P('dp', None), P('dp', None), P()), out_specs=(P('dp', None), P('dp', None), P('dp', None), P(None, None)), check_vma=False)
```

```python
import jax
import jax.numpy as jnp
from jax import lax
from jax.experimental import pallas as pl
from jax.experimental.pallas import tpu as pltpu
from jax.sharding import PartitionSpec as P

LAYERS = 2
MIX_RANK = 32
DECAY_RANK = 64
ADAM_STEP = 10

AXES = 3
UNITS = 7
CHUNKS = 4
SLOTS = 3
AHEAD = 4
PAIR_RING = 8
PIECE_ROWS = 256
FORWARD_ROWS = (512, 512, 512, 512)
LOAD_ROWS = 64
LOADS = 3
MESH = pl.DeviceIdType.MESH


def layout_runs(model_width, total_rows):
    ffn_width = 7 * model_width // 2
    layer_rows = 6 * model_width + 2 * ffn_width + 16 + 10 * MIX_RANK + 2 * DECAY_RANK
    vocab_rows = (total_rows - LAYERS * layer_rows - 4) // 2
    base_rule = (1.0, 0.0)
    decay_rule = (1.0, 0.1)
    time_rule = (2.0, 0.0)
    pieces = [(vocab_rows, decay_rule)]
    for layer_idx in range(LAYERS):
        lead_rows = 12 if layer_idx == 0 else 10
        pieces = pieces + [(lead_rows + 10 * MIX_RANK, base_rule), (1, time_rule), (2 * DECAY_RANK, base_rule), (1, time_rule), (5 * model_width, decay_rule), (4, base_rule), (2 * ffn_width + model_width, decay_rule)]
    pieces = pieces + [(2, base_rule), (vocab_rows, decay_rule)]
    run_starts = []
    next_row = 0
    for run_len, run_rule in pieces:
        run_starts.append(next_row)
        next_row = next_row + run_len
    lr_values = [run_rule[0] for run_len, run_rule in pieces]
    decay_values = [run_rule[1] for run_len, run_rule in pieces]
    return run_starts, lr_values, decay_values


def bit_flip(index, mask):
    flipped = index
    for bit in range(4):
        step = 1 << bit
        if mask & step:
            flipped = flipped + step - 2 * step * ((index // step) % 2)
    return flipped


def reduce_kernel(grads, g_out, c_out, pairs, landed, raw, stage, own_buf, pair_buf, part_buf, norm_buf,
                  pair_ssem, pair_rsem, send_sem, recv_sem, own_sem, pairl_sem, raw_ssem, raw_rsem, norm_sem, g_sem):
    me = lax.axis_index('dp')
    chip, core = me // 2, me % 2
    partner = bit_flip(me, 1)
    rows = g_out.shape[0]
    third = g_out.shape[1] // AXES
    part_rows = rows // CHUNKS
    devices = norm_buf.shape[0]

    def unit_row(j, k, parity):
        flip = chip
        e = 7 - j - (j + 4) // 7
        for place in range(AXES):
            step = 1 << ((k + place) % AXES)
            want = (e // (1 << (2 - place))) % 2
            bit = (chip // step) % 2
            flip = flip + want * (step - 2 * step * bit)
        return (2 * flip + parity) * rows

    def raw_copy(k, parity):
        owner = 2 * (bit_flip(me, 2 << k) // 2) + parity
        return pltpu.make_async_remote_copy(
            src_ref=grads.at[0, pl.ds(pl.multiple_of(owner * rows, rows), rows), pl.ds(k * third, third)],
            dst_ref=raw.at[k, core],
            send_sem=raw_ssem.at[k, parity],
            recv_sem=raw_rsem.at[k, core],
            device_id=(owner,),
            device_id_type=MESH)

    def raw_recv(k, parity):
        return pltpu.make_async_remote_copy(
            src_ref=grads.at[0, pl.ds(0, rows), pl.ds(k * third, third)],
            dst_ref=raw.at[k, parity],
            send_sem=raw_ssem.at[k, parity],
            recv_sem=raw_rsem.at[k, parity],
            device_id=(partner,),
            device_id_type=MESH)

    def pair_copy(s, k):
        j, i = s // CHUNKS, s % CHUNKS
        row = pl.multiple_of(unit_row(j, k, 1 - core) + i * part_rows, part_rows)
        return pltpu.make_async_remote_copy(
            src_ref=grads.at[0, pl.ds(row, part_rows), pl.ds(k * third, third)],
            dst_ref=pairs.at[j, k, pl.ds(pl.multiple_of(i * part_rows, part_rows), part_rows)],
            send_sem=pair_ssem.at[k],
            recv_sem=pair_rsem.at[s % PAIR_RING, k],
            device_id=(partner,),
            device_id_type=MESH)

    def own_load(s, k):
        j, i = s // CHUNKS, s % CHUNKS
        row = pl.multiple_of(unit_row(j, k, core) + i * part_rows, part_rows)
        return pltpu.make_async_copy(
            grads.at[0, pl.ds(row, part_rows), pl.ds(k * third, third)], own_buf.at[s % 2, k], own_sem.at[s % 2, k])

    def pair_load(s, k):
        j, i = s // CHUNKS, s % CHUNKS
        return pltpu.make_async_copy(
            pairs.at[j, k, pl.ds(pl.multiple_of(i * part_rows, part_rows), part_rows)], pair_buf.at[s % 2, k], pairl_sem.at[s % 2, k])

    def piece_copy(j, i, k, slot, axis):
        return pltpu.make_async_remote_copy(
            src_ref=stage.at[k, slot],
            dst_ref=landed.at[j, k, pl.ds(pl.multiple_of(i * part_rows, part_rows), part_rows)],
            send_sem=send_sem.at[k, slot],
            recv_sem=recv_sem.at[j, k, i],
            device_id=(bit_flip(me, 2 << axis),),
            device_id_type=MESH)

    total_steps = UNITS * CHUNKS

    def start_pairs(s):
        for k in range(AXES):
            pair_copy(s, k).start()

    def start_own(s):
        for k in range(AXES):
            own_load(s, k).start()

    def start_pair_loads(s):
        for k in range(AXES):
            pair_copy(s, k).wait_recv()
            pair_load(s, k).start()

    barrier = pltpu.get_barrier_semaphore()
    peers = [partner]
    for k in range(AXES):
        across = 2 * (bit_flip(me, 2 << k) // 2)
        peers += [across, across + 1]
    for peer in peers:
        pl.semaphore_signal(barrier, inc=1, device_id=(peer,), device_id_type=MESH)
    start_own(0)
    pl.semaphore_wait(barrier, len(peers))
    for parity in range(2):
        for k in range(AXES):
            raw_copy(k, parity).start()
    for s in range(AHEAD):
        start_pairs(s)
    start_pair_loads(0)

    def step(s, phase):
        j, i = s // CHUNKS, s % CHUNKS

        @pl.when(s + AHEAD < total_steps)
        def _():
            start_pairs(s + AHEAD)

        @pl.when(s + 1 < total_steps)
        def _():
            start_own(s + 1)

        def load_next():
            @pl.when(s + 1 < total_steps)
            def _():
                start_pair_loads(s + 1)

        if phase == 1:
            sources = []
        elif phase == 2:
            sources = [j - 3]
        elif phase == 3:
            sources = [2, 3]
        else:
            sources = [4, 5]
        slot = s % SLOTS
        base = pl.multiple_of(i * part_rows, part_rows)
        for k in range(AXES):
            own_load(s, k).wait()
            pair_load(s, k).wait()
            for source in sources:
                piece_copy(source, i, k, 0, 0).wait_recv()
            if phase < 4:
                @pl.when(s >= SLOTS)
                def _():
                    piece_copy(0, 0, k, slot, 0).wait_send()
            group = 64

            def add_rows(r, carry):
                lo = pl.multiple_of(r * group, group)
                value = own_buf[s % 2, k, pl.ds(lo, group)].astype(jnp.float32) + pair_buf[s % 2, k, pl.ds(lo, group)].astype(jnp.float32)
                for source in sources:
                    value = value + landed[source, k, pl.ds(base + lo, group)]
                if phase < 4:
                    stage[k, slot, pl.ds(lo, group)] = value
                    return carry
                for parity in range(2):
                    value = value + raw[k, parity, pl.ds(base + lo, group)].astype(jnp.float32)
                value = value * (1.0 / devices)
                landed[0, k, pl.ds(base + lo, group)] = value
                return carry + jnp.sum((value * value).reshape(group // 8, 8, third), axis=0)

            if phase < 4:
                lax.fori_loop(0, part_rows // group, add_rows, 0)
            else:
                part_buf[...] += lax.fori_loop(0, part_rows // group, add_rows, jnp.zeros((8, third), jnp.float32))
            if phase < 4:
                piece_copy(j, i, k, slot, (k + phase - 1) % AXES).start()
            else:
                pltpu.make_async_copy(
                    landed.at[0, k, pl.ds(base, part_rows)],
                    g_out.at[pl.ds(base, part_rows), pl.ds(k * third, third)], g_sem.at[k]).start()
        load_next()

    def pairs_sent(k):
        return pltpu.make_async_remote_copy(
            src_ref=pairs.at[:, k], dst_ref=pairs.at[:, k], send_sem=pair_ssem.at[k], recv_sem=pair_rsem.at[0, k],
            device_id=(partner,), device_id_type=MESH)

    part_buf[...] = jnp.zeros_like(part_buf)
    for phase, lo, hi in ((1, 0, 3), (2, 3, 5), (3, 5, 6), (4, 6, 7)):
        def run(s, carry, phase=phase):
            step(s, phase)
            return carry
        if phase == 4:
            for k in range(AXES):
                pairs_sent(k).wait_send()
            for k in range(AXES):
                for parity in range(2):
                    raw_recv(k, parity).wait_recv()
                    raw_copy(k, parity).wait_send()
        lax.fori_loop(lo * CHUNKS, hi * CHUNKS, run, 0)

    part_buf[:, :128] = part_buf[:, :128] + part_buf[:, 128:]
    norm_buf[me] = part_buf[:, :128]

    def norm_copy(d):
        return pltpu.make_async_remote_copy(
            src_ref=part_buf.at[:, pl.ds(0, 128)],
            dst_ref=norm_buf.at[me],
            send_sem=norm_sem.at[0],
            recv_sem=norm_sem.at[1],
            device_id=((me + d) % devices,),
            device_id_type=MESH)

    norm_all = pltpu.make_async_remote_copy(
        src_ref=norm_buf.at[pl.ds(1, devices - 1)], dst_ref=norm_buf.at[pl.ds(1, devices - 1)],
        send_sem=norm_sem.at[0], recv_sem=norm_sem.at[1], device_id=(partner,), device_id_type=MESH)

    for d in range(1, devices):
        norm_copy(d).start()
    for last in range(SLOTS):
        for k in range(AXES):
            piece_copy(0, 0, k, last, 0).wait_send()
    for k in range(AXES):
        pltpu.make_async_copy(landed.at[0, k], g_out.at[:, pl.ds(k * third, third)], g_sem.at[k]).wait()
    norm_all.wait_send()
    norm_all.wait_recv()
    square_sum = jnp.sum(jnp.sum(norm_buf[...], axis=0), keepdims=True)
    c_out[...] = jnp.broadcast_to(jnp.minimum(1.0, 1.0 / (jnp.sqrt(square_sum) + 1e-6)), c_out.shape)


def reduce_scatter(local_grads, devices):
    total_rows, width = local_grads.shape[1:]
    rows, third = total_rows // devices, width // AXES
    any_spec = pl.BlockSpec(memory_space=pl.ANY)
    f32, bf16 = jnp.float32, jnp.bfloat16
    part_rows = rows // CHUNKS
    g, scale, _ = pl.pallas_call(
        reduce_kernel,
        out_shape=(jax.ShapeDtypeStruct((rows, width), f32),
                   jax.ShapeDtypeStruct((8, 128), f32),
                   jax.ShapeDtypeStruct((UNITS, AXES, rows, third), bf16)),
        in_specs=[any_spec],
        out_specs=(any_spec, pl.BlockSpec(memory_space=pltpu.VMEM), any_spec),
        scratch_shapes=[
            pltpu.VMEM((UNITS - 1, AXES, rows, third), f32),
            pltpu.VMEM((AXES, 2, rows, third), bf16),
            pltpu.VMEM((AXES, SLOTS, part_rows, third), f32),
            pltpu.VMEM((2, AXES, part_rows, third), bf16),
            pltpu.VMEM((2, AXES, part_rows, third), bf16),
            pltpu.VMEM((8, third), f32),
            pltpu.VMEM((devices, 8, 128), f32),
            pltpu.SemaphoreType.DMA((AXES,)),
            pltpu.SemaphoreType.DMA((PAIR_RING, AXES)),
            pltpu.SemaphoreType.DMA((AXES, SLOTS)),
            pltpu.SemaphoreType.DMA((UNITS - 1, AXES, CHUNKS)),
            pltpu.SemaphoreType.DMA((2, AXES)),
            pltpu.SemaphoreType.DMA((2, AXES)),
            pltpu.SemaphoreType.DMA((AXES, 2)),
            pltpu.SemaphoreType.DMA((AXES, 2)),
            pltpu.SemaphoreType.DMA((2,)),
            pltpu.SemaphoreType.DMA((AXES,)),
        ],
        compiler_params=pltpu.CompilerParams(has_side_effects=True, vmem_limit_bytes=60 * 1024 * 1024, collective_id=0),
        name='reduce',
    )(local_grads)
    return g, scale


def update_gather_kernel(grad, master, first, second, scale, rate, working, new_master, new_first, new_second,
                         in_buf, out_buf, in_sem, out_sem, own_ssem, own_rsem, fwd_ssem, fwd_rsem, pair_ssem, pair_rsem):
    me = lax.axis_index('dp')
    partner = bit_flip(me, 1)
    rows, width = grad.shape
    third = width // AXES
    total_rows = working.shape[0]
    pieces = rows // PIECE_ROWS
    inputs = (grad, master, first, second)

    def piece_at(owner, i, cols, piece_rows):
        return working.at[pl.ds(pl.multiple_of(owner * rows + i * piece_rows, piece_rows), piece_rows), cols]

    def send(owner, i, cols, ssem, rsem, target, piece_rows=PIECE_ROWS):
        ref = piece_at(owner, i, cols, piece_rows)
        return pltpu.make_async_remote_copy(src_ref=ref, dst_ref=ref, send_sem=ssem, recv_sem=rsem,
                                            device_id=(target,), device_id_type=MESH)

    every = pl.ds(0, width)

    def cols_of(k):
        return pl.ds((k % AXES) * third, third)

    def chip_flip(*axes):
        mask = 0
        for axis in axes:
            mask ^= 2 << (axis % AXES)
        return bit_flip(me, mask)

    def load(t, n):
        here = pl.ds(pl.multiple_of(t * LOAD_ROWS, LOAD_ROWS), LOAD_ROWS)
        return pltpu.make_async_copy(inputs[n].at[here], in_buf.at[t % LOADS, n], in_sem.at[t % LOADS, n])

    def store(t):
        here = pl.ds(pl.multiple_of(t * LOAD_ROWS, LOAD_ROWS), LOAD_ROWS)
        return pltpu.make_async_copy(out_buf.at[t % 2], new_second.at[here], out_sem.at[t % 2])

    def own_send(i, axis):
        return send(me, i, every, own_ssem.at[axis], own_rsem.at[axis, i], chip_flip(axis))

    def own_recv(i, axis):
        return send(chip_flip(axis), i, every, own_ssem.at[axis], own_rsem.at[axis, i], chip_flip(axis))

    hops = (((0,), 1), ((0,), 2), ((1,), 2), ((0, 1), 2))

    def fwd_send(i, kind, k):
        source, axis = hops[kind]
        return send(chip_flip(*[k + a for a in source]), i, cols_of(k), fwd_ssem.at[kind], fwd_rsem.at[kind, k, i], chip_flip(k + axis), FORWARD_ROWS[kind])

    def fwd_recv(i, kind, k):
        source, axis = hops[kind]
        return send(chip_flip(*[k + a for a in source], k + axis), i, cols_of(k), fwd_ssem.at[kind], fwd_rsem.at[kind, k, i], chip_flip(k + axis), FORWARD_ROWS[kind])

    def pair_own(i):
        return send(me, i, every, pair_ssem.at[0], pair_rsem.at[0], partner)

    def pair_axis(i, axis):
        return send(chip_flip(axis), i, every, pair_ssem.at[1 + axis], pair_rsem.at[1 + axis], partner)

    def pair_fwd(i, kind, k):
        source, axis = hops[kind]
        owner = chip_flip(*[k + a for a in source], k + axis)
        return send(owner, i, cols_of(k), pair_ssem.at[4 + kind], pair_rsem.at[4 + kind], partner, FORWARD_ROWS[kind])

    def whole(ssem, rsem):
        return send(me, 0, every, ssem, rsem, partner, rows)

    clip = scale[0, 0]
    learn_rate = rate[0]
    run_starts, lr_values, decay_values = layout_runs(width, total_rows)
    first_norm = 1.0 / (1.0 - 0.9 ** ADAM_STEP)
    second_norm = 1.0 / (1.0 - 0.99 ** ADAM_STEP)

    steps = rows // LOAD_ROWS
    barrier = pltpu.get_barrier_semaphore()
    peers = [partner] + [chip_flip(axis) for axis in range(AXES)]
    for peer in peers:
        pl.semaphore_signal(barrier, inc=1, device_id=(peer,), device_id_type=MESH)
    for t in range(LOADS):
        for n in range(4):
            load(t, n).start()
    def update_rows(t, carry):
        for n in range(4):
            load(t, n).wait()

        @pl.when(t >= 2)
        def _():
            store(t - 2).wait()
        slot = t % LOADS
        out_slot = t % 2
        group = 16

        def group_step(r, carry):
            lo = pl.multiple_of(r * group, group)
            here = pl.ds(lo, group)
            row = pl.multiple_of(t * LOAD_ROWS + lo, group)
            start = me * rows + row
            row_ids = start + lax.broadcasted_iota(jnp.int32, (group, 128), 0)
            factor = jnp.full((group, 128), lr_values[0], jnp.float32)
            decay = jnp.full((group, 128), decay_values[0], jnp.float32)
            for r_start, r_lr, r_decay in zip(run_starts[1:], lr_values[1:], decay_values[1:]):
                past = row_ids >= r_start
                factor = jnp.where(past, r_lr, factor)
                decay = jnp.where(past, r_decay, decay)
            step_size = learn_rate * factor
            for tile in range(width // 128):
                at = pl.ds(tile * 128, 128)
                clipped = in_buf[slot, 0, here, at] * clip
                weights = in_buf[slot, 1, here, at]
                moment = 0.9 * in_buf[slot, 2, here, at] + 0.1 * clipped
                square = 0.99 * in_buf[slot, 3, here, at] + 0.01 * (clipped * clipped)
                moved = weights - step_size * ((moment * first_norm) / (jnp.sqrt(square * second_norm) + 1e-8) + decay * weights)
                new_master[pl.ds(row, group), at] = moved
                new_first[pl.ds(row, group), at] = moment
                out_buf[out_slot, here, at] = square
                working[pl.ds(pl.multiple_of(start, group), group), at] = moved.astype(jnp.bfloat16)
            return carry

        lax.fori_loop(0, LOAD_ROWS // group, group_step, 0)
        store(t).start()

        @pl.when(t + LOADS < steps)
        def _():
            for n in range(4):
                load(t + LOADS, n).start()
        return carry

    def own_piece(i, carry):
        per = PIECE_ROWS // LOAD_ROWS
        lax.fori_loop(i * per, (i + 1) * per, update_rows, 0)

        @pl.when(i == 0)
        def _():
            pl.semaphore_wait(barrier, len(peers))
        for axis in range(AXES):
            own_send(i, axis).start()
        pair_own(i).start()
        return carry

    def neighbour_piece(i, carry):
        per = FORWARD_ROWS[0] // PIECE_ROWS
        for part in range(per):
            for axis in range(AXES):
                own_recv(i * per + part, axis).wait_recv()
                pair_axis(i * per + part, axis).start()
        for kind in range(3):
            for k in range(AXES):
                fwd_send(i, kind, k).start()
        return carry

    def far_piece(i, carry):
        per = FORWARD_ROWS[0] // FORWARD_ROWS[3]
        for k in range(AXES):
            fwd_recv(i, 0, k).wait_recv()
            for part in range(per):
                fwd_send(i * per + part, 3, k).start()
            pair_fwd(i, 0, k).start()
        for kind in (1, 2):
            for k in range(AXES):
                fwd_recv(i, kind, k).wait_recv()
                pair_fwd(i, kind, k).start()
        return carry

    def last_piece(i, carry):
        for k in range(AXES):
            fwd_recv(i, 3, k).wait_recv()
            pair_fwd(i, 3, k).start()
        return carry

    def drain_own():
        for axis in range(AXES):
            whole(own_ssem.at[axis], own_rsem.at[axis, 0]).wait_send()
        for slot in range(4):
            whole(pair_ssem.at[slot], pair_rsem.at[slot]).wait_send()
            whole(pair_ssem.at[slot], pair_rsem.at[slot]).wait_recv()

    def drain_fwd(kinds):
        for kind in kinds:
            whole(fwd_ssem.at[kind], fwd_rsem.at[kind, 0, 0]).wait_send()
            whole(pair_ssem.at[4 + kind], pair_rsem.at[4 + kind]).wait_send()
            whole(pair_ssem.at[4 + kind], pair_rsem.at[4 + kind]).wait_recv()

    near_pieces, far_pieces = rows // FORWARD_ROWS[0], rows // FORWARD_ROWS[3]
    lax.fori_loop(0, pieces, own_piece, 0)
    lax.fori_loop(0, near_pieces, neighbour_piece, 0)
    for t in (steps - 2, steps - 1):
        store(t).wait()
    drain_own()
    lax.fori_loop(0, near_pieces, far_piece, 0)
    drain_fwd((0, 1, 2))
    lax.fori_loop(0, far_pieces, last_piece, 0)
    drain_fwd((3,))


def write_kernel(working, new_master, new_first, new_second, working_out, master_out, first_out, second_out,
                 buf, put_sem, in_sem, out_sem):
    rows = new_second.shape[0]
    slots, piece = buf.shape[:2]
    steps = rows // piece

    def load(s):
        return pltpu.make_async_copy(new_second.at[pl.ds(s * piece, piece)], buf.at[s % slots], in_sem.at[s % slots])

    def store(s):
        return pltpu.make_async_copy(buf.at[s % slots], second_out.at[pl.ds(s * piece, piece)], out_sem.at[s % slots])

    puts = [pltpu.make_async_copy(new_master, master_out, put_sem.at[0]), pltpu.make_async_copy(new_first, first_out, put_sem.at[1])]
    stripes = put_sem.shape[0] - 2
    stripe = working.shape[0] // stripes
    for n in range(stripes):
        here = pl.ds(n * stripe, stripe)
        puts.append(pltpu.make_async_copy(working.at[here], working_out.at[here], put_sem.at[n + 2]))

    for s in range(slots):
        load(s).start()
    for s in range(steps):
        for put in puts[s * len(puts) // steps:(s + 1) * len(puts) // steps]:
            put.start()
        load(s).wait()
        store(s).start()
        if s + 1 >= slots and s + 1 < steps:
            store(s + 1 - slots).wait()
            load(s + 1).start()
    for s in range(steps - slots, steps):
        store(s).wait()
    for put in puts:
        put.wait()


def update_gather(grad, master, first, second, scale, rate, devices):
    rows, width = grad.shape
    any_spec = pl.BlockSpec(memory_space=pltpu.HBM)
    vmem_spec = pl.BlockSpec(memory_space=pltpu.VMEM)
    f32, bf16 = jnp.float32, jnp.bfloat16
    pieces = rows // PIECE_ROWS
    shard = pltpu.HBM((rows, width), f32)
    near = pltpu.VMEM((rows, width), f32)
    dma = pltpu.SemaphoreType.DMA
    working, new_master, new_first, new_second = pl.pallas_call(
        update_gather_kernel,
        out_shape=(pltpu.VMEM((devices * rows, width), bf16), near, near, shard),
        in_specs=[any_spec] * 4 + [vmem_spec, pl.BlockSpec(memory_space=pltpu.SMEM)],
        out_specs=(vmem_spec, vmem_spec, vmem_spec, any_spec),
        scratch_shapes=[
            pltpu.VMEM((LOADS, 4, LOAD_ROWS, width), f32),
            pltpu.VMEM((2, LOAD_ROWS, width), f32),
            dma((LOADS, 4)),
            dma((2,)),
            dma((AXES,)),
            dma((AXES, pieces)),
            dma((4,)),
            dma((4, AXES, rows // min(FORWARD_ROWS))),
            dma((8,)),
            dma((8,)),
        ],
        compiler_params=pltpu.CompilerParams(has_side_effects=True, vmem_limit_bytes=3 * 1024 * 1024, collective_id=1),
        name='gather',
    )(grad, master, first, second, scale, rate.reshape(1))
    working_shape = pltpu.HBM((devices * rows, width), bf16)
    return pl.pallas_call(
        write_kernel,
        out_shape=(working_shape, shard, shard, shard),
        in_specs=[vmem_spec, vmem_spec, vmem_spec, any_spec],
        out_specs=(any_spec,) * 4,
        scratch_shapes=[pltpu.VMEM((3, rows // 8, width), f32), dma((18,)), dma((3,)), dma((3,))],
        compiler_params=pltpu.CompilerParams(vmem_limit_bytes=3 * 1024 * 1024),
        name='write',
    )(*[pltpu.with_memory_space_constraint(x, pltpu.VMEM) for x in (working, new_master, new_first)], new_second)


def solution(mesh):
    dev_count = mesh.shape['dp']

    def device_step(local_grads, master, mom_first, mom_second, learn_rate):
        grad_shard, clip_scale = reduce_scatter(local_grads, dev_count)
        working, new_master, new_first, new_second = update_gather(grad_shard, master, mom_first, mom_second, clip_scale, learn_rate, dev_count)
        return new_master, new_first, new_second, working

    return jax.shard_map(device_step, mesh=mesh, in_specs=(P('dp', None, None), P('dp', None), P('dp', None), P('dp', None), P()), out_specs=(P('dp', None), P('dp', None), P('dp', None), P(None, None)), check_vma=False)
```

```python
import jax
import jax.numpy as jnp
from jax import lax
from jax.experimental import pallas as pl
from jax.experimental.pallas import tpu as pltpu
from jax.sharding import PartitionSpec as P

LAYERS = 2
MIX_RANK = 32
DECAY_RANK = 64
ADAM_STEP = 10

AXES = 3
UNITS = 7
CHUNKS = 4
SUBS = 2
SLOTS = 3
AHEAD = 4
PAIR_RING = 8
PIECE_ROWS = 256
FORWARD_ROWS = (512, 512, 512, 256)
LOAD_ROWS = 32
LOADS = 6
MESH = pl.DeviceIdType.MESH


def layout_runs(model_width, total_rows):
    ffn_width = 7 * model_width // 2
    layer_rows = 6 * model_width + 2 * ffn_width + 16 + 10 * MIX_RANK + 2 * DECAY_RANK
    vocab_rows = (total_rows - LAYERS * layer_rows - 4) // 2
    base_rule = (1.0, 0.0)
    decay_rule = (1.0, 0.1)
    time_rule = (2.0, 0.0)
    pieces = [(vocab_rows, decay_rule)]
    for layer_idx in range(LAYERS):
        lead_rows = 12 if layer_idx == 0 else 10
        pieces = pieces + [(lead_rows + 10 * MIX_RANK, base_rule), (1, time_rule), (2 * DECAY_RANK, base_rule), (1, time_rule), (5 * model_width, decay_rule), (4, base_rule), (2 * ffn_width + model_width, decay_rule)]
    pieces = pieces + [(2, base_rule), (vocab_rows, decay_rule)]
    run_starts = []
    next_row = 0
    for run_len, run_rule in pieces:
        run_starts.append(next_row)
        next_row = next_row + run_len
    lr_values = [run_rule[0] for run_len, run_rule in pieces]
    decay_values = [run_rule[1] for run_len, run_rule in pieces]
    return run_starts, lr_values, decay_values


def bit_flip(index, mask):
    flipped = index
    for bit in range(4):
        step = 1 << bit
        if mask & step:
            flipped = flipped + step - 2 * step * ((index // step) % 2)
    return flipped


def reduce_kernel(grads, g_out, c_out, pairs, landed, raw, stage, own_buf, pair_buf, part_buf, norm_buf,
                  pair_ssem, pair_rsem, send_sem, recv_sem, last_sem, own_sem, pairl_sem, raw_ssem, raw_rsem, norm_sem, g_sem):
    me = lax.axis_index('dp')
    chip, core = me // 2, me % 2
    partner = bit_flip(me, 1)
    rows = g_out.shape[0]
    third = g_out.shape[1] // AXES
    part_rows = rows // CHUNKS
    devices = norm_buf.shape[0]

    def unit_row(j, k, parity):
        flip = chip
        e = 7 - j - (j + 4) // 7
        for place in range(AXES):
            step = 1 << ((k + place) % AXES)
            want = (e // (1 << (2 - place))) % 2
            bit = (chip // step) % 2
            flip = flip + want * (step - 2 * step * bit)
        return (2 * flip + parity) * rows

    def raw_copy(k, parity):
        owner = 2 * (bit_flip(me, 2 << k) // 2) + parity
        return pltpu.make_async_remote_copy(
            src_ref=grads.at[0, pl.ds(pl.multiple_of(owner * rows, rows), rows), pl.ds(k * third, third)],
            dst_ref=raw.at[k, core],
            send_sem=raw_ssem.at[k, parity],
            recv_sem=raw_rsem.at[k, core],
            device_id=(owner,),
            device_id_type=MESH)

    def raw_recv(k, parity):
        return pltpu.make_async_remote_copy(
            src_ref=grads.at[0, pl.ds(0, rows), pl.ds(k * third, third)],
            dst_ref=raw.at[k, parity],
            send_sem=raw_ssem.at[k, parity],
            recv_sem=raw_rsem.at[k, parity],
            device_id=(partner,),
            device_id_type=MESH)

    def pair_copy(s, k):
        j, i = s // CHUNKS, s % CHUNKS
        row = pl.multiple_of(unit_row(j, k, 1 - core) + i * part_rows, part_rows)
        return pltpu.make_async_remote_copy(
            src_ref=grads.at[0, pl.ds(row, part_rows), pl.ds(k * third, third)],
            dst_ref=pairs.at[j, k, pl.ds(pl.multiple_of(i * part_rows, part_rows), part_rows)],
            send_sem=pair_ssem.at[k],
            recv_sem=pair_rsem.at[s % PAIR_RING, k],
            device_id=(partner,),
            device_id_type=MESH)

    def own_load(s, k):
        j, i = s // CHUNKS, s % CHUNKS
        row = pl.multiple_of(unit_row(j, k, core) + i * part_rows, part_rows)
        return pltpu.make_async_copy(
            grads.at[0, pl.ds(row, part_rows), pl.ds(k * third, third)], own_buf.at[s % 2, k], own_sem.at[s % 2, k])

    def pair_load(s, k):
        j, i = s // CHUNKS, s % CHUNKS
        return pltpu.make_async_copy(
            pairs.at[j, k, pl.ds(pl.multiple_of(i * part_rows, part_rows), part_rows)], pair_buf.at[s % 2, k], pairl_sem.at[s % 2, k])

    sub_rows = part_rows // SUBS

    def piece_copy(j, i, k, slot, axis):
        return pltpu.make_async_remote_copy(
            src_ref=stage.at[k, slot],
            dst_ref=landed.at[j, k, pl.ds(pl.multiple_of(i * part_rows, part_rows), part_rows)],
            send_sem=send_sem.at[k, slot],
            recv_sem=recv_sem.at[j, k],
            device_id=(bit_flip(me, 2 << axis),),
            device_id_type=MESH)

    def last_copy(i, sub, k, slot, axis):
        return pltpu.make_async_remote_copy(
            src_ref=stage.at[k, slot, pl.ds(sub * sub_rows, sub_rows)],
            dst_ref=landed.at[UNITS - 2, k, pl.ds(pl.multiple_of(i * part_rows + sub * sub_rows, sub_rows), sub_rows)],
            send_sem=send_sem.at[k, slot],
            recv_sem=last_sem.at[k, i, sub],
            device_id=(bit_flip(me, 2 << axis),),
            device_id_type=MESH)

    def unit_recv(j, k):
        return pltpu.make_async_remote_copy(
            src_ref=landed.at[j, k], dst_ref=landed.at[j, k], send_sem=send_sem.at[k, 0], recv_sem=recv_sem.at[j, k],
            device_id=(partner,), device_id_type=MESH)

    total_steps = UNITS * CHUNKS

    def start_pairs(s):
        for k in range(AXES):
            pair_copy(s, k).start()

    def start_own(s):
        for k in range(AXES):
            own_load(s, k).start()

    def start_pair_loads(s):
        for k in range(AXES):
            pair_copy(s, k).wait_recv()
            pair_load(s, k).start()

    barrier = pltpu.get_barrier_semaphore()
    peers = [partner]
    for k in range(AXES):
        across = 2 * (bit_flip(me, 2 << k) // 2)
        peers += [across, across + 1]
    for peer in peers:
        pl.semaphore_signal(barrier, inc=1, device_id=(peer,), device_id_type=MESH)
    start_own(0)
    pl.semaphore_wait(barrier, len(peers))
    for parity in range(2):
        for k in range(AXES):
            raw_copy(k, parity).start()
    for s in range(AHEAD):
        start_pairs(s)
    start_pair_loads(0)

    def step(s, phase):
        j, i = s // CHUNKS, s % CHUNKS

        @pl.when(s + AHEAD < total_steps)
        def _():
            start_pairs(s + AHEAD)

        @pl.when(s + 1 < total_steps)
        def _():
            start_own(s + 1)

        def load_next():
            @pl.when(s + 1 < total_steps)
            def _():
                start_pair_loads(s + 1)

        if phase == 1:
            sources = []
        elif phase == 2:
            sources = [j - 3]
        elif phase == 3:
            sources = [2, 3]
        else:
            sources = [4, 5]
        slot = s % SLOTS
        base = pl.multiple_of(i * part_rows, part_rows)
        for k in range(AXES):
            own_load(s, k).wait()
            pair_load(s, k).wait()
            if phase < 4:
                @pl.when(s >= SLOTS)
                def _():
                    piece_copy(0, 0, k, slot, 0).wait_send()
        subs = SUBS if phase > 2 else 1
        count = part_rows // subs
        group = 64
        for sub in range(subs):
            for k in range(AXES):
                if phase == 4:
                    last_copy(i, sub, k, 0, 0).wait_recv()

                def add_rows(r, carry):
                    lo = pl.multiple_of(sub * count + r * group, group)
                    value = own_buf[s % 2, k, pl.ds(lo, group)].astype(jnp.float32) + pair_buf[s % 2, k, pl.ds(lo, group)].astype(jnp.float32)
                    for source in sources:
                        value = value + landed[source, k, pl.ds(base + lo, group)]
                    if phase < 4:
                        stage[k, slot, pl.ds(lo, group)] = value
                        return carry
                    for parity in range(2):
                        value = value + raw[k, parity, pl.ds(base + lo, group)].astype(jnp.float32)
                    value = value * (1.0 / devices)
                    landed[0, k, pl.ds(base + lo, group)] = value
                    return carry + jnp.sum((value * value).reshape(group // 8, 8, third), axis=0)

                if phase < 4:
                    lax.fori_loop(0, count // group, add_rows, 0)
                else:
                    part_buf[...] += lax.fori_loop(0, count // group, add_rows, jnp.zeros((8, third), jnp.float32))
                if phase < 3:
                    piece_copy(j, i, k, slot, (k + phase - 1) % AXES).start()
                elif phase == 3:
                    last_copy(i, sub, k, slot, (k + phase - 1) % AXES).start()
        if phase == 4:
            for k in range(AXES):
                pltpu.make_async_copy(
                    landed.at[0, k, pl.ds(base, part_rows)],
                    g_out.at[pl.ds(base, part_rows), pl.ds(k * third, third)], g_sem.at[k]).start()
        load_next()

    def pairs_sent(k):
        return pltpu.make_async_remote_copy(
            src_ref=pairs.at[:, k], dst_ref=pairs.at[:, k], send_sem=pair_ssem.at[k], recv_sem=pair_rsem.at[0, k],
            device_id=(partner,), device_id_type=MESH)

    part_buf[...] = jnp.zeros_like(part_buf)
    for phase, lo, hi in ((1, 0, 3), (2, 3, 5), (3, 5, 6), (4, 6, 7)):
        def run(s, carry, phase=phase):
            step(s, phase)
            return carry
        for source in ([], [0, 1], [2, 3], [4])[phase - 1]:
            for k in range(AXES):
                unit_recv(source, k).wait_recv()
        if phase == 4:
            for k in range(AXES):
                pairs_sent(k).wait_send()
            for k in range(AXES):
                for parity in range(2):
                    raw_recv(k, parity).wait_recv()
                    raw_copy(k, parity).wait_send()
        lax.fori_loop(lo * CHUNKS, hi * CHUNKS, run, 0)

    part_buf[:, :128] = part_buf[:, :128] + part_buf[:, 128:]
    norm_buf[me] = part_buf[:, :128]

    def norm_copy(d):
        return pltpu.make_async_remote_copy(
            src_ref=part_buf.at[:, pl.ds(0, 128)],
            dst_ref=norm_buf.at[me],
            send_sem=norm_sem.at[0],
            recv_sem=norm_sem.at[1],
            device_id=((me + d) % devices,),
            device_id_type=MESH)

    norm_all = pltpu.make_async_remote_copy(
        src_ref=norm_buf.at[pl.ds(1, devices - 1)], dst_ref=norm_buf.at[pl.ds(1, devices - 1)],
        send_sem=norm_sem.at[0], recv_sem=norm_sem.at[1], device_id=(partner,), device_id_type=MESH)

    for d in range(1, devices):
        norm_copy(d).start()
    for last in range(SLOTS):
        for k in range(AXES):
            piece_copy(0, 0, k, last, 0).wait_send()
    for k in range(AXES):
        pltpu.make_async_copy(landed.at[0, k], g_out.at[:, pl.ds(k * third, third)], g_sem.at[k]).wait()
    norm_all.wait_send()
    norm_all.wait_recv()
    square_sum = jnp.sum(jnp.sum(norm_buf[...], axis=0), keepdims=True)
    c_out[...] = jnp.broadcast_to(jnp.minimum(1.0, 1.0 / (jnp.sqrt(square_sum) + 1e-6)), c_out.shape)


def reduce_scatter(local_grads, devices):
    total_rows, width = local_grads.shape[1:]
    rows, third = total_rows // devices, width // AXES
    any_spec = pl.BlockSpec(memory_space=pl.ANY)
    f32, bf16 = jnp.float32, jnp.bfloat16
    part_rows = rows // CHUNKS
    g, scale, _ = pl.pallas_call(
        reduce_kernel,
        out_shape=(jax.ShapeDtypeStruct((rows, width), f32),
                   jax.ShapeDtypeStruct((8, 128), f32),
                   jax.ShapeDtypeStruct((UNITS, AXES, rows, third), bf16)),
        in_specs=[any_spec],
        out_specs=(any_spec, pl.BlockSpec(memory_space=pltpu.VMEM), any_spec),
        scratch_shapes=[
            pltpu.VMEM((UNITS - 1, AXES, rows, third), f32),
            pltpu.VMEM((AXES, 2, rows, third), bf16),
            pltpu.VMEM((AXES, SLOTS, part_rows, third), f32),
            pltpu.VMEM((2, AXES, part_rows, third), bf16),
            pltpu.VMEM((2, AXES, part_rows, third), bf16),
            pltpu.VMEM((8, third), f32),
            pltpu.VMEM((devices, 8, 128), f32),
            pltpu.SemaphoreType.DMA((AXES,)),
            pltpu.SemaphoreType.DMA((PAIR_RING, AXES)),
            pltpu.SemaphoreType.DMA((AXES, SLOTS)),
            pltpu.SemaphoreType.DMA((UNITS - 2, AXES)),
            pltpu.SemaphoreType.DMA((AXES, CHUNKS, SUBS)),
            pltpu.SemaphoreType.DMA((2, AXES)),
            pltpu.SemaphoreType.DMA((2, AXES)),
            pltpu.SemaphoreType.DMA((AXES, 2)),
            pltpu.SemaphoreType.DMA((AXES, 2)),
            pltpu.SemaphoreType.DMA((2,)),
            pltpu.SemaphoreType.DMA((AXES,)),
        ],
        compiler_params=pltpu.CompilerParams(has_side_effects=True, vmem_limit_bytes=60 * 1024 * 1024, collective_id=0),
        name='reduce',
    )(local_grads)
    return g, scale


def update_gather_kernel(grad, master, first, second, scale, rate, working, new_master, new_first, new_second,
                         in_buf, out_buf, in_sem, out_sem, own_ssem, own_rsem, fwd_ssem, fwd_rsem, pair_ssem, pair_rsem):
    me = lax.axis_index('dp')
    partner = bit_flip(me, 1)
    rows, width = grad.shape
    third = width // AXES
    total_rows = working.shape[0]
    pieces = rows // PIECE_ROWS
    inputs = (grad, master, first, second)

    def piece_at(owner, i, cols, piece_rows):
        return working.at[pl.ds(pl.multiple_of(owner * rows + i * piece_rows, piece_rows), piece_rows), cols]

    def first_send(t, axis):
        return send(me, t, every, own_ssem.at[axis], own_rsem.at[axis, 0], chip_flip(axis), LOAD_ROWS)

    def send(owner, i, cols, ssem, rsem, target, piece_rows=PIECE_ROWS):
        ref = piece_at(owner, i, cols, piece_rows)
        return pltpu.make_async_remote_copy(src_ref=ref, dst_ref=ref, send_sem=ssem, recv_sem=rsem,
                                            device_id=(target,), device_id_type=MESH)

    every = pl.ds(0, width)

    def cols_of(k):
        return pl.ds((k % AXES) * third, third)

    def chip_flip(*axes):
        mask = 0
        for axis in axes:
            mask ^= 2 << (axis % AXES)
        return bit_flip(me, mask)

    def load(t, n):
        here = pl.ds(pl.multiple_of(t * LOAD_ROWS, LOAD_ROWS), LOAD_ROWS)
        return pltpu.make_async_copy(inputs[n].at[here], in_buf.at[t % LOADS, n], in_sem.at[t % LOADS, n])

    def store(t):
        here = pl.ds(pl.multiple_of(t * LOAD_ROWS, LOAD_ROWS), LOAD_ROWS)
        return pltpu.make_async_copy(out_buf.at[t % 2], new_second.at[here], out_sem.at[t % 2])

    def own_send(i, axis):
        return send(me, i, every, own_ssem.at[axis], own_rsem.at[axis, i], chip_flip(axis))

    def own_recv(i, axis):
        return send(chip_flip(axis), i, every, own_ssem.at[axis], own_rsem.at[axis, i], chip_flip(axis))

    hops = (((0,), 1), ((0,), 2), ((1,), 2), ((0, 1), 2))

    def fwd_send(i, kind, k):
        source, axis = hops[kind]
        return send(chip_flip(*[k + a for a in source]), i, cols_of(k), fwd_ssem.at[kind], fwd_rsem.at[kind, k, i], chip_flip(k + axis), FORWARD_ROWS[kind])

    def fwd_recv(i, kind, k):
        source, axis = hops[kind]
        return send(chip_flip(*[k + a for a in source], k + axis), i, cols_of(k), fwd_ssem.at[kind], fwd_rsem.at[kind, k, i], chip_flip(k + axis), FORWARD_ROWS[kind])

    def pair_own(i):
        return send(me, i, every, pair_ssem.at[0], pair_rsem.at[0], partner)

    def pair_axis(i, axis):
        return send(chip_flip(axis), i, every, pair_ssem.at[1 + axis], pair_rsem.at[1 + axis], partner)

    def pair_fwd(i, kind, k):
        source, axis = hops[kind]
        owner = chip_flip(*[k + a for a in source], k + axis)
        return send(owner, i, cols_of(k), pair_ssem.at[4 + kind], pair_rsem.at[4 + kind], partner, FORWARD_ROWS[kind])

    def whole(ssem, rsem):
        return send(me, 0, every, ssem, rsem, partner, rows)

    clip = scale[0, 0]
    learn_rate = rate[0]
    run_starts, lr_values, decay_values = layout_runs(width, total_rows)
    first_norm = 1.0 / (1.0 - 0.9 ** ADAM_STEP)
    second_norm = 1.0 / (1.0 - 0.99 ** ADAM_STEP)

    steps = rows // LOAD_ROWS
    barrier = pltpu.get_barrier_semaphore()
    peers = [partner] + [chip_flip(axis) for axis in range(AXES)]
    for peer in peers:
        pl.semaphore_signal(barrier, inc=1, device_id=(peer,), device_id_type=MESH)
    for t in range(LOADS):
        for n in range(4):
            load(t, n).start()
    def update_rows(t, carry):
        for n in range(4):
            load(t, n).wait()

        @pl.when(t >= 2)
        def _():
            store(t - 2).wait()
        slot = t % LOADS
        out_slot = t % 2
        group = 16

        def group_step(r, carry):
            lo = pl.multiple_of(r * group, group)
            here = pl.ds(lo, group)
            row = pl.multiple_of(t * LOAD_ROWS + lo, group)
            start = me * rows + row
            row_ids = start + lax.broadcasted_iota(jnp.int32, (group, 128), 0)
            factor = jnp.full((group, 128), lr_values[0], jnp.float32)
            decay = jnp.full((group, 128), decay_values[0], jnp.float32)
            for r_start, r_lr, r_decay in zip(run_starts[1:], lr_values[1:], decay_values[1:]):
                past = row_ids >= r_start
                factor = jnp.where(past, r_lr, factor)
                decay = jnp.where(past, r_decay, decay)
            step_size = learn_rate * factor
            for tile in range(width // 128):
                at = pl.ds(tile * 128, 128)
                clipped = in_buf[slot, 0, here, at] * clip
                weights = in_buf[slot, 1, here, at]
                moment = 0.9 * in_buf[slot, 2, here, at] + 0.1 * clipped
                square = 0.99 * in_buf[slot, 3, here, at] + 0.01 * (clipped * clipped)
                moved = weights - step_size * ((moment * first_norm) / (jnp.sqrt(square * second_norm) + 1e-8) + decay * weights)
                new_master[pl.ds(row, group), at] = moved
                new_first[pl.ds(row, group), at] = moment
                out_buf[out_slot, here, at] = square
                working[pl.ds(pl.multiple_of(start, group), group), at] = moved.astype(jnp.bfloat16)
            return carry

        lax.fori_loop(0, LOAD_ROWS // group, group_step, 0)
        store(t).start()

        @pl.when(t + LOADS < steps)
        def _():
            for n in range(4):
                load(t + LOADS, n).start()
        return carry

    def own_piece(i, carry):
        per = PIECE_ROWS // LOAD_ROWS
        lax.fori_loop(i * per, (i + 1) * per, update_rows, 0)
        for axis in range(AXES):
            own_send(i, axis).start()
        pair_own(i).start()
        return carry

    def neighbour_piece(i, carry):
        per = FORWARD_ROWS[0] // PIECE_ROWS
        for part in range(per):
            for axis in range(AXES):
                own_recv(i * per + part, axis).wait_recv()
                pair_axis(i * per + part, axis).start()
        for kind in range(3):
            for k in range(AXES):
                fwd_send(i, kind, k).start()
        return carry

    def far_piece(i, carry):
        per = FORWARD_ROWS[0] // FORWARD_ROWS[3]
        for k in range(AXES):
            fwd_recv(i, 0, k).wait_recv()
            for part in range(per):
                fwd_send(i * per + part, 3, k).start()
            pair_fwd(i, 0, k).start()
        for kind in (1, 2):
            for k in range(AXES):
                fwd_recv(i, kind, k).wait_recv()
                pair_fwd(i, kind, k).start()
        return carry

    def last_piece(i, carry):
        for k in range(AXES):
            fwd_recv(i, 3, k).wait_recv()
            pair_fwd(i, 3, k).start()
        return carry

    def drain_own():
        for axis in range(AXES):
            whole(own_ssem.at[axis], own_rsem.at[axis, 0]).wait_send()
        for slot in range(4):
            whole(pair_ssem.at[slot], pair_rsem.at[slot]).wait_send()
            whole(pair_ssem.at[slot], pair_rsem.at[slot]).wait_recv()

    def drain_fwd(kinds):
        for kind in kinds:
            whole(fwd_ssem.at[kind], fwd_rsem.at[kind, 0, 0]).wait_send()
            whole(pair_ssem.at[4 + kind], pair_rsem.at[4 + kind]).wait_send()
            whole(pair_ssem.at[4 + kind], pair_rsem.at[4 + kind]).wait_recv()

    near_pieces, far_pieces = rows // FORWARD_ROWS[0], rows // FORWARD_ROWS[3]
    for t in range(PIECE_ROWS // LOAD_ROWS):
        update_rows(t, 0)
        if t == 0:
            pl.semaphore_wait(barrier, len(peers))
        for axis in range(AXES):
            first_send(t, axis).start()
    pair_own(0).start()
    lax.fori_loop(1, pieces, own_piece, 0)
    lax.fori_loop(0, near_pieces, neighbour_piece, 0)
    for t in (steps - 2, steps - 1):
        store(t).wait()
    drain_own()
    lax.fori_loop(0, near_pieces, far_piece, 0)
    drain_fwd((0, 1, 2))
    lax.fori_loop(0, far_pieces, last_piece, 0)
    drain_fwd((3,))


def write_kernel(working, new_master, new_first, new_second, working_out, master_out, first_out, second_out,
                 buf, put_sem, in_sem, out_sem):
    rows = new_second.shape[0]
    slots, piece = buf.shape[:2]
    steps = rows // piece

    def load(s):
        return pltpu.make_async_copy(new_second.at[pl.ds(s * piece, piece)], buf.at[s % slots], in_sem.at[s % slots])

    def store(s):
        return pltpu.make_async_copy(buf.at[s % slots], second_out.at[pl.ds(s * piece, piece)], out_sem.at[s % slots])

    puts = [pltpu.make_async_copy(new_master, master_out, put_sem.at[0]), pltpu.make_async_copy(new_first, first_out, put_sem.at[1])]
    stripes = put_sem.shape[0] - 2
    stripe = working.shape[0] // stripes
    for n in range(stripes):
        here = pl.ds(n * stripe, stripe)
        puts.append(pltpu.make_async_copy(working.at[here], working_out.at[here], put_sem.at[n + 2]))

    for s in range(slots):
        load(s).start()
    for s in range(steps):
        for put in puts[s * len(puts) // steps:(s + 1) * len(puts) // steps]:
            put.start()
        load(s).wait()
        store(s).start()
        if s + 1 >= slots and s + 1 < steps:
            store(s + 1 - slots).wait()
            load(s + 1).start()
    for s in range(steps - slots, steps):
        store(s).wait()
    for put in puts:
        put.wait()


def update_gather(grad, master, first, second, scale, rate, devices):
    rows, width = grad.shape
    any_spec = pl.BlockSpec(memory_space=pltpu.HBM)
    vmem_spec = pl.BlockSpec(memory_space=pltpu.VMEM)
    f32, bf16 = jnp.float32, jnp.bfloat16
    pieces = rows // PIECE_ROWS
    shard = pltpu.HBM((rows, width), f32)
    near = pltpu.VMEM((rows, width), f32)
    dma = pltpu.SemaphoreType.DMA
    working, new_master, new_first, new_second = pl.pallas_call(
        update_gather_kernel,
        out_shape=(pltpu.VMEM((devices * rows, width), bf16), near, near, shard),
        in_specs=[any_spec] * 4 + [vmem_spec, pl.BlockSpec(memory_space=pltpu.SMEM)],
        out_specs=(vmem_spec, vmem_spec, vmem_spec, any_spec),
        scratch_shapes=[
            pltpu.VMEM((LOADS, 4, LOAD_ROWS, width), f32),
            pltpu.VMEM((2, LOAD_ROWS, width), f32),
            dma((LOADS, 4)),
            dma((2,)),
            dma((AXES,)),
            dma((AXES, pieces)),
            dma((4,)),
            dma((4, AXES, rows // min(FORWARD_ROWS))),
            dma((8,)),
            dma((8,)),
        ],
        compiler_params=pltpu.CompilerParams(has_side_effects=True, vmem_limit_bytes=3 * 1024 * 1024, collective_id=1),
        name='gather',
    )(grad, master, first, second, scale, rate.reshape(1))
    working_shape = pltpu.HBM((devices * rows, width), bf16)
    return pl.pallas_call(
        write_kernel,
        out_shape=(working_shape, shard, shard, shard),
        in_specs=[vmem_spec, vmem_spec, vmem_spec, any_spec],
        out_specs=(any_spec,) * 4,
        scratch_shapes=[pltpu.VMEM((3, rows // 8, width), f32), dma((18,)), dma((3,)), dma((3,))],
        compiler_params=pltpu.CompilerParams(vmem_limit_bytes=3 * 1024 * 1024),
        name='write',
    )(*[pltpu.with_memory_space_constraint(x, pltpu.VMEM) for x in (working, new_master, new_first)], new_second)


def solution(mesh):
    dev_count = mesh.shape['dp']

    def device_step(local_grads, master, mom_first, mom_second, learn_rate):
        grad_shard, clip_scale = reduce_scatter(local_grads, dev_count)
        working, new_master, new_first, new_second = update_gather(grad_shard, master, mom_first, mom_second, clip_scale, learn_rate, dev_count)
        return new_master, new_first, new_second, working

    return jax.shard_map(device_step, mesh=mesh, in_specs=(P('dp', None, None), P('dp', None), P('dp', None), P('dp', None), P()), out_specs=(P('dp', None), P('dp', None), P('dp', None), P(None, None)), check_vma=False)
```

```python
import jax
import jax.numpy as jnp
from jax import lax
from jax.experimental import pallas as pl
from jax.experimental.pallas import tpu as pltpu
from jax.sharding import PartitionSpec as P

LAYERS = 2
MIX_RANK = 32
DECAY_RANK = 64
ADAM_STEP = 10

AXES = 3
UNITS = 7
CHUNKS = 4
SUBS = 2
SLOTS = 3
AHEAD = 4
PAIR_RING = 8
PIECE_ROWS = 256
FORWARD_ROWS = (512, 512, 512, 256)
LOAD_ROWS = 32
LOADS = 6
MESH = pl.DeviceIdType.MESH


def layout_runs(model_width, total_rows):
    ffn_width = 7 * model_width // 2
    layer_rows = 6 * model_width + 2 * ffn_width + 16 + 10 * MIX_RANK + 2 * DECAY_RANK
    vocab_rows = (total_rows - LAYERS * layer_rows - 4) // 2
    base_rule = (1.0, 0.0)
    decay_rule = (1.0, 0.1)
    time_rule = (2.0, 0.0)
    pieces = [(vocab_rows, decay_rule)]
    for layer_idx in range(LAYERS):
        lead_rows = 12 if layer_idx == 0 else 10
        pieces = pieces + [(lead_rows + 10 * MIX_RANK, base_rule), (1, time_rule), (2 * DECAY_RANK, base_rule), (1, time_rule), (5 * model_width, decay_rule), (4, base_rule), (2 * ffn_width + model_width, decay_rule)]
    pieces = pieces + [(2, base_rule), (vocab_rows, decay_rule)]
    run_starts = []
    next_row = 0
    for run_len, run_rule in pieces:
        run_starts.append(next_row)
        next_row = next_row + run_len
    lr_values = [run_rule[0] for run_len, run_rule in pieces]
    decay_values = [run_rule[1] for run_len, run_rule in pieces]
    return run_starts, lr_values, decay_values


def bit_flip(index, mask):
    flipped = index
    for bit in range(4):
        step = 1 << bit
        if mask & step:
            flipped = flipped + step - 2 * step * ((index // step) % 2)
    return flipped


def reduce_kernel(grads, g_out, c_out, pairs, landed, raw, stage, own_buf, pair_buf, part_buf, norm_buf,
                  pair_ssem, pair_rsem, send_sem, recv_sem, last_sem, own_sem, pairl_sem, raw_ssem, raw_rsem, norm_sem, g_sem):
    me = lax.axis_index('dp')
    chip, core = me // 2, me % 2
    partner = bit_flip(me, 1)
    rows = g_out.shape[0]
    third = g_out.shape[1] // AXES
    part_rows = rows // CHUNKS
    devices = norm_buf.shape[0]

    def unit_row(j, k, parity):
        flip = chip
        e = 7 - j - (j + 4) // 7
        for place in range(AXES):
            step = 1 << ((k + place) % AXES)
            want = (e // (1 << (2 - place))) % 2
            bit = (chip // step) % 2
            flip = flip + want * (step - 2 * step * bit)
        return (2 * flip + parity) * rows

    def raw_copy(k, parity):
        owner = 2 * (bit_flip(me, 2 << k) // 2) + parity
        return pltpu.make_async_remote_copy(
            src_ref=grads.at[0, pl.ds(pl.multiple_of(owner * rows, rows), rows), pl.ds(k * third, third)],
            dst_ref=raw.at[k, core],
            send_sem=raw_ssem.at[k, parity],
            recv_sem=raw_rsem.at[k, core],
            device_id=(owner,),
            device_id_type=MESH)

    def raw_recv(k, parity):
        return pltpu.make_async_remote_copy(
            src_ref=grads.at[0, pl.ds(0, rows), pl.ds(k * third, third)],
            dst_ref=raw.at[k, parity],
            send_sem=raw_ssem.at[k, parity],
            recv_sem=raw_rsem.at[k, parity],
            device_id=(partner,),
            device_id_type=MESH)

    def pair_copy(s, k):
        j, i = s // CHUNKS, s % CHUNKS
        row = pl.multiple_of(unit_row(j, k, 1 - core) + i * part_rows, part_rows)
        return pltpu.make_async_remote_copy(
            src_ref=grads.at[0, pl.ds(row, part_rows), pl.ds(k * third, third)],
            dst_ref=pairs.at[j, k, pl.ds(pl.multiple_of(i * part_rows, part_rows), part_rows)],
            send_sem=pair_ssem.at[k],
            recv_sem=pair_rsem.at[s % PAIR_RING, k],
            device_id=(partner,),
            device_id_type=MESH)

    def own_load(s, k):
        j, i = s // CHUNKS, s % CHUNKS
        row = pl.multiple_of(unit_row(j, k, core) + i * part_rows, part_rows)
        return pltpu.make_async_copy(
            grads.at[0, pl.ds(row, part_rows), pl.ds(k * third, third)], own_buf.at[s % 2, k], own_sem.at[s % 2, k])

    def pair_load(s, k):
        j, i = s // CHUNKS, s % CHUNKS
        return pltpu.make_async_copy(
            pairs.at[j, k, pl.ds(pl.multiple_of(i * part_rows, part_rows), part_rows)], pair_buf.at[s % 2, k], pairl_sem.at[s % 2, k])

    sub_rows = part_rows // SUBS

    def piece_copy(j, i, k, slot, axis):
        return pltpu.make_async_remote_copy(
            src_ref=stage.at[k, slot],
            dst_ref=landed.at[j, k, pl.ds(pl.multiple_of(i * part_rows, part_rows), part_rows)],
            send_sem=send_sem.at[k, slot],
            recv_sem=recv_sem.at[j, k],
            device_id=(bit_flip(me, 2 << axis),),
            device_id_type=MESH)

    def last_copy(i, sub, k, slot, axis):
        return pltpu.make_async_remote_copy(
            src_ref=stage.at[k, slot, pl.ds(sub * sub_rows, sub_rows)],
            dst_ref=landed.at[UNITS - 2, k, pl.ds(pl.multiple_of(i * part_rows + sub * sub_rows, sub_rows), sub_rows)],
            send_sem=send_sem.at[k, slot],
            recv_sem=last_sem.at[k, i, sub],
            device_id=(bit_flip(me, 2 << axis),),
            device_id_type=MESH)

    def unit_recv(j, k):
        return pltpu.make_async_remote_copy(
            src_ref=landed.at[j, k], dst_ref=landed.at[j, k], send_sem=send_sem.at[k, 0], recv_sem=recv_sem.at[j, k],
            device_id=(partner,), device_id_type=MESH)

    total_steps = UNITS * CHUNKS

    def start_pairs(s):
        for k in range(AXES):
            pair_copy(s, k).start()

    def start_own(s):
        for k in range(AXES):
            own_load(s, k).start()

    def start_pair_loads(s):
        for k in range(AXES):
            pair_copy(s, k).wait_recv()
            pair_load(s, k).start()

    barrier = pltpu.get_barrier_semaphore()
    peers = [partner]
    for k in range(AXES):
        across = 2 * (bit_flip(me, 2 << k) // 2)
        peers += [across, across + 1]
    for peer in peers:
        pl.semaphore_signal(barrier, inc=1, device_id=(peer,), device_id_type=MESH)
    start_own(0)
    pl.semaphore_wait(barrier, len(peers))
    for parity in range(2):
        for k in range(AXES):
            raw_copy(k, parity).start()
    for s in range(AHEAD):
        start_pairs(s)
    start_pair_loads(0)

    def step(s, phase):
        j, i = s // CHUNKS, s % CHUNKS

        @pl.when(s + AHEAD < total_steps)
        def _():
            start_pairs(s + AHEAD)

        @pl.when(s + 1 < total_steps)
        def _():
            start_own(s + 1)

        def load_next():
            @pl.when(s + 1 < total_steps)
            def _():
                start_pair_loads(s + 1)

        if phase == 1:
            sources = []
        elif phase == 2:
            sources = [j - 3]
        elif phase == 3:
            sources = [2, 3]
        else:
            sources = [4, 5]
        slot = s % SLOTS
        base = pl.multiple_of(i * part_rows, part_rows)
        for k in range(AXES):
            own_load(s, k).wait()
            pair_load(s, k).wait()
            if phase < 4:
                @pl.when(s >= SLOTS)
                def _():
                    piece_copy(0, 0, k, slot, 0).wait_send()
        subs = SUBS if phase > 2 else 1
        count = part_rows // subs
        group = 64
        for sub in range(subs):
            for k in range(AXES):
                if phase == 4:
                    last_copy(i, sub, k, 0, 0).wait_recv()

                def add_rows(r, carry):
                    lo = pl.multiple_of(sub * count + r * group, group)
                    value = own_buf[s % 2, k, pl.ds(lo, group)].astype(jnp.float32) + pair_buf[s % 2, k, pl.ds(lo, group)].astype(jnp.float32)
                    for source in sources:
                        value = value + landed[source, k, pl.ds(base + lo, group)]
                    if phase < 4:
                        stage[k, slot, pl.ds(lo, group)] = value
                        return carry
                    for parity in range(2):
                        value = value + raw[k, parity, pl.ds(base + lo, group)].astype(jnp.float32)
                    value = value * (1.0 / devices)
                    landed[0, k, pl.ds(base + lo, group)] = value
                    return carry + jnp.sum((value * value).reshape(group // 8, 8, third), axis=0)

                if phase < 4:
                    lax.fori_loop(0, count // group, add_rows, 0)
                else:
                    part_buf[...] += lax.fori_loop(0, count // group, add_rows, jnp.zeros((8, third), jnp.float32))
                if phase < 3:
                    piece_copy(j, i, k, slot, (k + phase - 1) % AXES).start()
                elif phase == 3:
                    last_copy(i, sub, k, slot, (k + phase - 1) % AXES).start()
        if phase == 4:
            for k in range(AXES):
                pltpu.make_async_copy(
                    landed.at[0, k, pl.ds(base, part_rows)],
                    g_out.at[pl.ds(base, part_rows), pl.ds(k * third, third)], g_sem.at[k]).start()
        load_next()

    def pairs_sent(k):
        return pltpu.make_async_remote_copy(
            src_ref=pairs.at[:, k], dst_ref=pairs.at[:, k], send_sem=pair_ssem.at[k], recv_sem=pair_rsem.at[0, k],
            device_id=(partner,), device_id_type=MESH)

    part_buf[...] = jnp.zeros_like(part_buf)
    for phase, lo, hi in ((1, 0, 3), (2, 3, 5), (3, 5, 6), (4, 6, 7)):
        def run(s, carry, phase=phase):
            step(s, phase)
            return carry
        for source in ([], [0, 1], [2, 3], [4])[phase - 1]:
            for k in range(AXES):
                unit_recv(source, k).wait_recv()
        if phase == 4:
            for k in range(AXES):
                pairs_sent(k).wait_send()
            for k in range(AXES):
                for parity in range(2):
                    raw_recv(k, parity).wait_recv()
                    raw_copy(k, parity).wait_send()
        lax.fori_loop(lo * CHUNKS, hi * CHUNKS, run, 0)

    part_buf[:, :128] = part_buf[:, :128] + part_buf[:, 128:]
    norm_buf[me] = part_buf[:, :128]

    def norm_copy(d):
        return pltpu.make_async_remote_copy(
            src_ref=part_buf.at[:, pl.ds(0, 128)],
            dst_ref=norm_buf.at[me],
            send_sem=norm_sem.at[0],
            recv_sem=norm_sem.at[1],
            device_id=(bit_flip(me, d),),
            device_id_type=MESH)

    norm_all = pltpu.make_async_remote_copy(
        src_ref=norm_buf.at[pl.ds(1, devices - 1)], dst_ref=norm_buf.at[pl.ds(1, devices - 1)],
        send_sem=norm_sem.at[0], recv_sem=norm_sem.at[1], device_id=(partner,), device_id_type=MESH)

    for d in sorted(range(1, devices), key=lambda d: -bin(d // 2).count('1')):
        norm_copy(d).start()
    for last in range(SLOTS):
        for k in range(AXES):
            piece_copy(0, 0, k, last, 0).wait_send()
    for k in range(AXES):
        pltpu.make_async_copy(landed.at[0, k], g_out.at[:, pl.ds(k * third, third)], g_sem.at[k]).wait()
    norm_all.wait_send()
    norm_all.wait_recv()
    square_sum = jnp.sum(jnp.sum(norm_buf[...], axis=0), keepdims=True)
    c_out[...] = jnp.broadcast_to(jnp.minimum(1.0, 1.0 / (jnp.sqrt(square_sum) + 1e-6)), c_out.shape)


def reduce_scatter(local_grads, devices):
    total_rows, width = local_grads.shape[1:]
    rows, third = total_rows // devices, width // AXES
    any_spec = pl.BlockSpec(memory_space=pl.ANY)
    f32, bf16 = jnp.float32, jnp.bfloat16
    part_rows = rows // CHUNKS
    g, scale, _ = pl.pallas_call(
        reduce_kernel,
        out_shape=(jax.ShapeDtypeStruct((rows, width), f32),
                   jax.ShapeDtypeStruct((8, 128), f32),
                   jax.ShapeDtypeStruct((UNITS, AXES, rows, third), bf16)),
        in_specs=[any_spec],
        out_specs=(any_spec, pl.BlockSpec(memory_space=pltpu.VMEM), any_spec),
        scratch_shapes=[
            pltpu.VMEM((UNITS - 1, AXES, rows, third), f32),
            pltpu.VMEM((AXES, 2, rows, third), bf16),
            pltpu.VMEM((AXES, SLOTS, part_rows, third), f32),
            pltpu.VMEM((2, AXES, part_rows, third), bf16),
            pltpu.VMEM((2, AXES, part_rows, third), bf16),
            pltpu.VMEM((8, third), f32),
            pltpu.VMEM((devices, 8, 128), f32),
            pltpu.SemaphoreType.DMA((AXES,)),
            pltpu.SemaphoreType.DMA((PAIR_RING, AXES)),
            pltpu.SemaphoreType.DMA((AXES, SLOTS)),
            pltpu.SemaphoreType.DMA((UNITS - 2, AXES)),
            pltpu.SemaphoreType.DMA((AXES, CHUNKS, SUBS)),
            pltpu.SemaphoreType.DMA((2, AXES)),
            pltpu.SemaphoreType.DMA((2, AXES)),
            pltpu.SemaphoreType.DMA((AXES, 2)),
            pltpu.SemaphoreType.DMA((AXES, 2)),
            pltpu.SemaphoreType.DMA((2,)),
            pltpu.SemaphoreType.DMA((AXES,)),
        ],
        compiler_params=pltpu.CompilerParams(has_side_effects=True, vmem_limit_bytes=60 * 1024 * 1024, collective_id=0),
        name='reduce',
    )(local_grads)
    return g, scale


def update_gather_kernel(grad, master, first, second, scale, rate, working, new_master, new_first, new_second,
                         in_buf, out_buf, rate_buf, scale_buf, small_sem, in_sem, out_sem, own_ssem, own_rsem, fwd_ssem, fwd_rsem, pair_ssem, pair_rsem):
    me = lax.axis_index('dp')
    partner = bit_flip(me, 1)
    rows, width = grad.shape
    third = width // AXES
    total_rows = working.shape[0]
    pieces = rows // PIECE_ROWS
    inputs = (grad, master, first, second)

    def piece_at(owner, i, cols, piece_rows):
        return working.at[pl.ds(pl.multiple_of(owner * rows + i * piece_rows, piece_rows), piece_rows), cols]

    def first_send(t, axis):
        return send(me, t, every, own_ssem.at[axis], own_rsem.at[axis, 0], chip_flip(axis), LOAD_ROWS)

    def send(owner, i, cols, ssem, rsem, target, piece_rows=PIECE_ROWS):
        ref = piece_at(owner, i, cols, piece_rows)
        return pltpu.make_async_remote_copy(src_ref=ref, dst_ref=ref, send_sem=ssem, recv_sem=rsem,
                                            device_id=(target,), device_id_type=MESH)

    every = pl.ds(0, width)

    def cols_of(k):
        return pl.ds((k % AXES) * third, third)

    def chip_flip(*axes):
        mask = 0
        for axis in axes:
            mask ^= 2 << (axis % AXES)
        return bit_flip(me, mask)

    def load(t, n):
        here = pl.ds(pl.multiple_of(t * LOAD_ROWS, LOAD_ROWS), LOAD_ROWS)
        return pltpu.make_async_copy(inputs[n].at[here], in_buf.at[t % LOADS, n], in_sem.at[t % LOADS, n])

    def store(t):
        here = pl.ds(pl.multiple_of(t * LOAD_ROWS, LOAD_ROWS), LOAD_ROWS)
        return pltpu.make_async_copy(out_buf.at[t % 2], new_second.at[here], out_sem.at[t % 2])

    def own_send(i, axis):
        return send(me, i, every, own_ssem.at[axis], own_rsem.at[axis, i], chip_flip(axis))

    def own_recv(i, axis):
        return send(chip_flip(axis), i, every, own_ssem.at[axis], own_rsem.at[axis, i], chip_flip(axis))

    fwd_base = [AXES * sum(rows // n for n in FORWARD_ROWS[:kind]) for kind in range(4)]
    hops = (((0,), 1), ((0,), 2), ((1,), 2), ((0, 1), 2))

    def fwd_send(i, kind, k):
        source, axis = hops[kind]
        return send(chip_flip(*[k + a for a in source]), i, cols_of(k), fwd_ssem.at[kind], fwd_rsem.at[fwd_base[kind] + k * (rows // FORWARD_ROWS[kind]) + i], chip_flip(k + axis), FORWARD_ROWS[kind])

    def fwd_recv(i, kind, k):
        source, axis = hops[kind]
        return send(chip_flip(*[k + a for a in source], k + axis), i, cols_of(k), fwd_ssem.at[kind], fwd_rsem.at[fwd_base[kind] + k * (rows // FORWARD_ROWS[kind]) + i], chip_flip(k + axis), FORWARD_ROWS[kind])

    def pair_own(i):
        return send(me, i, every, pair_ssem.at[0], pair_rsem.at[0], partner)

    def pair_axis(i, axis):
        return send(chip_flip(axis), i, every, pair_ssem.at[1 + axis], pair_rsem.at[1 + axis], partner)

    def pair_fwd(i, kind, k):
        source, axis = hops[kind]
        owner = chip_flip(*[k + a for a in source], k + axis)
        return send(owner, i, cols_of(k), pair_ssem.at[4 + kind], pair_rsem.at[4 + kind], partner, FORWARD_ROWS[kind])

    def whole(ssem, rsem):
        return send(me, 0, every, ssem, rsem, partner, rows)

    run_starts, lr_values, decay_values = layout_runs(width, total_rows)
    first_norm = 1.0 / (1.0 - 0.9 ** ADAM_STEP)
    second_norm = 1.0 / (1.0 - 0.99 ** ADAM_STEP)

    steps = rows // LOAD_ROWS
    small = (pltpu.make_async_copy(scale, scale_buf, small_sem.at[0]), pltpu.make_async_copy(rate, rate_buf, small_sem.at[1]))
    for copy in small:
        copy.start()
    barrier = pltpu.get_barrier_semaphore()
    peers = [partner] + [chip_flip(axis) for axis in range(AXES)]
    for peer in peers:
        pl.semaphore_signal(barrier, inc=1, device_id=(peer,), device_id_type=MESH)
    for t in range(LOADS):
        for n in range(4):
            load(t, n).start()
    def update_rows(t, carry):
        for n in range(4):
            load(t, n).wait()

        @pl.when(t >= 2)
        def _():
            store(t - 2).wait()
        slot = t % LOADS
        out_slot = t % 2
        group = 16

        def group_step(r, carry):
            lo = pl.multiple_of(r * group, group)
            here = pl.ds(lo, group)
            row = pl.multiple_of(t * LOAD_ROWS + lo, group)
            start = me * rows + row
            row_ids = start + lax.broadcasted_iota(jnp.int32, (group, 128), 0)
            factor = jnp.full((group, 128), lr_values[0], jnp.float32)
            decay = jnp.full((group, 128), decay_values[0], jnp.float32)
            for r_start, r_lr, r_decay in zip(run_starts[1:], lr_values[1:], decay_values[1:]):
                past = row_ids >= r_start
                factor = jnp.where(past, r_lr, factor)
                decay = jnp.where(past, r_decay, decay)
            step_size = rate_buf[...] * factor
            for tile in range(width // 128):
                at = pl.ds(tile * 128, 128)
                clipped = in_buf[slot, 0, here, at] * scale_buf[pl.ds(0, 1)]
                weights = in_buf[slot, 1, here, at]
                moment = 0.9 * in_buf[slot, 2, here, at] + 0.1 * clipped
                square = 0.99 * in_buf[slot, 3, here, at] + 0.01 * (clipped * clipped)
                moved = weights - step_size * ((moment * first_norm) / (jnp.sqrt(square * second_norm) + 1e-8) + decay * weights)
                new_master[pl.ds(row, group), at] = moved
                new_first[pl.ds(row, group), at] = moment
                out_buf[out_slot, here, at] = square
                working[pl.ds(pl.multiple_of(start, group), group), at] = moved.astype(jnp.bfloat16)
            return carry

        lax.fori_loop(0, LOAD_ROWS // group, group_step, 0)
        store(t).start()

        @pl.when(t + LOADS < steps)
        def _():
            for n in range(4):
                load(t + LOADS, n).start()
        return carry

    def own_piece(i, carry):
        per = PIECE_ROWS // LOAD_ROWS
        lax.fori_loop(i * per, (i + 1) * per, update_rows, 0)
        for axis in range(AXES):
            own_send(i, axis).start()
        pair_own(i).start()
        return carry

    def neighbour_piece(i, carry):
        per = FORWARD_ROWS[0] // PIECE_ROWS
        for part in range(per):
            for axis in range(AXES):
                own_recv(i * per + part, axis).wait_recv()
                pair_axis(i * per + part, axis).start()
        for kind in range(3):
            for k in range(AXES):
                fwd_send(i, kind, k).start()
        return carry

    def far_piece(i, carry):
        per = FORWARD_ROWS[0] // FORWARD_ROWS[3]
        for k in range(AXES):
            fwd_recv(i, 0, k).wait_recv()
            for part in range(per):
                fwd_send(i * per + part, 3, k).start()
            pair_fwd(i, 0, k).start()
        for kind in (1, 2):
            for k in range(AXES):
                fwd_recv(i, kind, k).wait_recv()
                pair_fwd(i, kind, k).start()
        return carry

    def last_piece(i, carry):
        for k in range(AXES):
            fwd_recv(i, 3, k).wait_recv()
            pair_fwd(i, 3, k).start()
        return carry

    def drain_own():
        for axis in range(AXES):
            whole(own_ssem.at[axis], own_rsem.at[axis, 0]).wait_send()
        for slot in range(4):
            whole(pair_ssem.at[slot], pair_rsem.at[slot]).wait_send()
            whole(pair_ssem.at[slot], pair_rsem.at[slot]).wait_recv()

    def drain_fwd(kinds):
        for kind in kinds:
            whole(fwd_ssem.at[kind], fwd_rsem.at[fwd_base[kind]]).wait_send()
            whole(pair_ssem.at[4 + kind], pair_rsem.at[4 + kind]).wait_send()
            whole(pair_ssem.at[4 + kind], pair_rsem.at[4 + kind]).wait_recv()

    near_pieces, far_pieces = rows // FORWARD_ROWS[0], rows // FORWARD_ROWS[3]
    for copy in small:
        copy.wait()
    for t in range(PIECE_ROWS // LOAD_ROWS):
        update_rows(t, 0)
        if t == 0:
            pl.semaphore_wait(barrier, len(peers))
        for axis in range(AXES):
            first_send(t, axis).start()
    pair_own(0).start()
    lax.fori_loop(1, pieces, own_piece, 0)
    lax.fori_loop(0, near_pieces, neighbour_piece, 0)
    for t in (steps - 2, steps - 1):
        store(t).wait()
    drain_own()
    lax.fori_loop(0, near_pieces, far_piece, 0)
    drain_fwd((0, 1, 2))
    lax.fori_loop(0, far_pieces, last_piece, 0)
    drain_fwd((3,))


def write_kernel(working, new_master, new_first, new_second, working_out, master_out, first_out, second_out,
                 buf, put_sem, in_sem, out_sem):
    rows = new_second.shape[0]
    slots, piece = buf.shape[:2]
    steps = rows // piece

    def load(s):
        return pltpu.make_async_copy(new_second.at[pl.ds(s * piece, piece)], buf.at[s % slots], in_sem.at[s % slots])

    def store(s):
        return pltpu.make_async_copy(buf.at[s % slots], second_out.at[pl.ds(s * piece, piece)], out_sem.at[s % slots])

    puts = [pltpu.make_async_copy(new_master, master_out, put_sem.at[0]), pltpu.make_async_copy(new_first, first_out, put_sem.at[1])]
    stripes = put_sem.shape[0] - 2
    stripe = working.shape[0] // stripes
    for n in range(stripes):
        here = pl.ds(n * stripe, stripe)
        puts.append(pltpu.make_async_copy(working.at[here], working_out.at[here], put_sem.at[n + 2]))

    for s in range(slots):
        load(s).start()
    for s in range(steps):
        for put in puts[s * len(puts) // steps:(s + 1) * len(puts) // steps]:
            put.start()
        load(s).wait()
        store(s).start()
        if s + 1 >= slots and s + 1 < steps:
            store(s + 1 - slots).wait()
            load(s + 1).start()
    for s in range(steps - slots, steps):
        store(s).wait()
    for put in puts:
        put.wait()


def update_gather(grad, master, first, second, scale, rate, devices):
    rows, width = grad.shape
    any_spec = pl.BlockSpec(memory_space=pltpu.HBM)
    vmem_spec = pl.BlockSpec(memory_space=pltpu.VMEM)
    f32, bf16 = jnp.float32, jnp.bfloat16
    pieces = rows // PIECE_ROWS
    shard = pltpu.HBM((rows, width), f32)
    near = pltpu.VMEM((rows, width), f32)
    dma = pltpu.SemaphoreType.DMA
    working, new_master, new_first, new_second = pl.pallas_call(
        update_gather_kernel,
        out_shape=(pltpu.VMEM((devices * rows, width), bf16), near, near, shard),
        in_specs=[any_spec] * 6,
        out_specs=(vmem_spec, vmem_spec, vmem_spec, any_spec),
        scratch_shapes=[
            pltpu.VMEM((LOADS, 4, LOAD_ROWS, width), f32),
            pltpu.VMEM((2, LOAD_ROWS, width), f32),
            pltpu.VMEM((1, 128), f32),
            pltpu.VMEM((8, 128), f32),
            dma((2,)),
            dma((LOADS, 4)),
            dma((2,)),
            dma((AXES,)),
            dma((AXES, pieces)),
            dma((4,)),
            dma((AXES * sum(rows // n for n in FORWARD_ROWS),)),
            dma((8,)),
            dma((8,)),
        ],
        compiler_params=pltpu.CompilerParams(has_side_effects=True, vmem_limit_bytes=3 * 1024 * 1024, collective_id=1),
        name='gather',
    )(grad, master, first, second, scale, jnp.broadcast_to(rate, (1, 128)))
    working_shape = pltpu.HBM((devices * rows, width), bf16)
    return pl.pallas_call(
        write_kernel,
        out_shape=(working_shape, shard, shard, shard),
        in_specs=[vmem_spec, vmem_spec, vmem_spec, any_spec],
        out_specs=(any_spec,) * 4,
        scratch_shapes=[pltpu.VMEM((3, rows // 8, width), f32), dma((18,)), dma((3,)), dma((3,))],
        compiler_params=pltpu.CompilerParams(vmem_limit_bytes=3 * 1024 * 1024),
        name='write',
    )(*[pltpu.with_memory_space_constraint(x, pltpu.VMEM) for x in (working, new_master, new_first)], new_second)


def solution(mesh):
    dev_count = mesh.shape['dp']

    def device_step(local_grads, master, mom_first, mom_second, learn_rate):
        grad_shard, clip_scale = reduce_scatter(local_grads, dev_count)
        working, new_master, new_first, new_second = update_gather(grad_shard, master, mom_first, mom_second, clip_scale, learn_rate, dev_count)
        return new_master, new_first, new_second, working

    return jax.shard_map(device_step, mesh=mesh, in_specs=(P('dp', None, None), P('dp', None), P('dp', None), P('dp', None), P()), out_specs=(P('dp', None), P('dp', None), P('dp', None), P(None, None)), check_vma=False)
```

```python
import jax
import jax.numpy as jnp
from jax import lax
from jax.experimental import pallas as pl
from jax.experimental.pallas import tpu as pltpu
from jax.sharding import PartitionSpec as P

LAYERS = 2
MIX_RANK = 32
DECAY_RANK = 64
ADAM_STEP = 10

AXES = 3
UNITS = 7
CHUNKS = 4
SUBS = 2
SLOTS = 3
AHEAD = 4
PAIR_RING = 8
PIECE_ROWS = 512
FORWARD_ROWS = (512, 512, 512, 256)
LOAD_ROWS = 32
LOADS = 6
MESH = pl.DeviceIdType.MESH


def layout_runs(model_width, total_rows):
    ffn_width = 7 * model_width // 2
    layer_rows = 6 * model_width + 2 * ffn_width + 16 + 10 * MIX_RANK + 2 * DECAY_RANK
    vocab_rows = (total_rows - LAYERS * layer_rows - 4) // 2
    base_rule = (1.0, 0.0)
    decay_rule = (1.0, 0.1)
    time_rule = (2.0, 0.0)
    pieces = [(vocab_rows, decay_rule)]
    for layer_idx in range(LAYERS):
        lead_rows = 12 if layer_idx == 0 else 10
        pieces = pieces + [(lead_rows + 10 * MIX_RANK, base_rule), (1, time_rule), (2 * DECAY_RANK, base_rule), (1, time_rule), (5 * model_width, decay_rule), (4, base_rule), (2 * ffn_width + model_width, decay_rule)]
    pieces = pieces + [(2, base_rule), (vocab_rows, decay_rule)]
    run_starts = []
    next_row = 0
    for run_len, run_rule in pieces:
        run_starts.append(next_row)
        next_row = next_row + run_len
    lr_values = [run_rule[0] for run_len, run_rule in pieces]
    decay_values = [run_rule[1] for run_len, run_rule in pieces]
    return run_starts, lr_values, decay_values


def bit_flip(index, mask):
    flipped = index
    for bit in range(4):
        step = 1 << bit
        if mask & step:
            flipped = flipped + step - 2 * step * ((index // step) % 2)
    return flipped


def reduce_kernel(grads, g_out, c_out, pairs, landed, raw, stage, own_buf, pair_buf, part_buf, norm_buf,
                  pair_ssem, pair_rsem, send_sem, recv_sem, last_sem, own_sem, pairl_sem, raw_ssem, raw_rsem, norm_sem, g_sem):
    me = lax.axis_index('dp')
    chip, core = me // 2, me % 2
    partner = bit_flip(me, 1)
    rows = g_out.shape[0]
    third = g_out.shape[1] // AXES
    part_rows = rows // CHUNKS
    devices = norm_buf.shape[0]

    def unit_row(j, k, parity):
        flip = chip
        e = 7 - j - (j + 4) // 7
        for place in range(AXES):
            step = 1 << ((k + place) % AXES)
            want = (e // (1 << (2 - place))) % 2
            bit = (chip // step) % 2
            flip = flip + want * (step - 2 * step * bit)
        return (2 * flip + parity) * rows

    def raw_copy(k, parity):
        owner = 2 * (bit_flip(me, 2 << k) // 2) + parity
        return pltpu.make_async_remote_copy(
            src_ref=grads.at[0, pl.ds(pl.multiple_of(owner * rows, rows), rows), pl.ds(k * third, third)],
            dst_ref=raw.at[k, core],
            send_sem=raw_ssem.at[k, parity],
            recv_sem=raw_rsem.at[k, core],
            device_id=(owner,),
            device_id_type=MESH)

    def raw_recv(k, parity):
        return pltpu.make_async_remote_copy(
            src_ref=grads.at[0, pl.ds(0, rows), pl.ds(k * third, third)],
            dst_ref=raw.at[k, parity],
            send_sem=raw_ssem.at[k, parity],
            recv_sem=raw_rsem.at[k, parity],
            device_id=(partner,),
            device_id_type=MESH)

    def pair_copy(s, k):
        j, i = s // CHUNKS, s % CHUNKS
        row = pl.multiple_of(unit_row(j, k, 1 - core) + i * part_rows, part_rows)
        return pltpu.make_async_remote_copy(
            src_ref=grads.at[0, pl.ds(row, part_rows), pl.ds(k * third, third)],
            dst_ref=pairs.at[j, k, pl.ds(pl.multiple_of(i * part_rows, part_rows), part_rows)],
            send_sem=pair_ssem.at[k],
            recv_sem=pair_rsem.at[s % PAIR_RING, k],
            device_id=(partner,),
            device_id_type=MESH)

    def own_load(s, k):
        j, i = s // CHUNKS, s % CHUNKS
        row = pl.multiple_of(unit_row(j, k, core) + i * part_rows, part_rows)
        return pltpu.make_async_copy(
            grads.at[0, pl.ds(row, part_rows), pl.ds(k * third, third)], own_buf.at[s % 2, k], own_sem.at[s % 2, k])

    def pair_load(s, k):
        j, i = s // CHUNKS, s % CHUNKS
        return pltpu.make_async_copy(
            pairs.at[j, k, pl.ds(pl.multiple_of(i * part_rows, part_rows), part_rows)], pair_buf.at[s % 2, k], pairl_sem.at[s % 2, k])

    sub_rows = part_rows // SUBS

    def piece_copy(j, i, k, slot, axis):
        return pltpu.make_async_remote_copy(
            src_ref=stage.at[k, slot],
            dst_ref=landed.at[j, k, pl.ds(pl.multiple_of(i * part_rows, part_rows), part_rows)],
            send_sem=send_sem.at[k, slot],
            recv_sem=recv_sem.at[j, k],
            device_id=(bit_flip(me, 2 << axis),),
            device_id_type=MESH)

    def last_copy(i, sub, k, slot, axis):
        return pltpu.make_async_remote_copy(
            src_ref=stage.at[k, slot, pl.ds(sub * sub_rows, sub_rows)],
            dst_ref=landed.at[UNITS - 2, k, pl.ds(pl.multiple_of(i * part_rows + sub * sub_rows, sub_rows), sub_rows)],
            send_sem=send_sem.at[k, slot],
            recv_sem=last_sem.at[k, i, sub],
            device_id=(bit_flip(me, 2 << axis),),
            device_id_type=MESH)

    def unit_recv(j, k):
        return pltpu.make_async_remote_copy(
            src_ref=landed.at[j, k], dst_ref=landed.at[j, k], send_sem=send_sem.at[k, 0], recv_sem=recv_sem.at[j, k],
            device_id=(partner,), device_id_type=MESH)

    total_steps = UNITS * CHUNKS

    def start_pairs(s):
        for k in range(AXES):
            pair_copy(s, k).start()

    def start_own(s):
        for k in range(AXES):
            own_load(s, k).start()

    def start_pair_loads(s):
        for k in range(AXES):
            pair_copy(s, k).wait_recv()
            pair_load(s, k).start()

    barrier = pltpu.get_barrier_semaphore()
    peers = [partner]
    for k in range(AXES):
        across = 2 * (bit_flip(me, 2 << k) // 2)
        peers += [across, across + 1]
    for peer in peers:
        pl.semaphore_signal(barrier, inc=1, device_id=(peer,), device_id_type=MESH)
    start_own(0)
    pl.semaphore_wait(barrier, len(peers))
    for parity in range(2):
        for k in range(AXES):
            raw_copy(k, parity).start()
    for s in range(AHEAD):
        start_pairs(s)
    start_pair_loads(0)

    def step(s, phase):
        j, i = s // CHUNKS, s % CHUNKS

        @pl.when(s + AHEAD < total_steps)
        def _():
            start_pairs(s + AHEAD)

        @pl.when(s + 1 < total_steps)
        def _():
            start_own(s + 1)

        def load_next():
            @pl.when(s + 1 < total_steps)
            def _():
                start_pair_loads(s + 1)

        if phase == 1:
            sources = []
        elif phase == 2:
            sources = [j - 3]
        elif phase == 3:
            sources = [2, 3]
        else:
            sources = [4, 5]
        slot = s % SLOTS
        base = pl.multiple_of(i * part_rows, part_rows)
        for k in range(AXES):
            own_load(s, k).wait()
            pair_load(s, k).wait()
            if phase < 4:
                @pl.when(s >= SLOTS)
                def _():
                    piece_copy(0, 0, k, slot, 0).wait_send()
        subs = SUBS if phase > 2 else 1
        count = part_rows // subs
        group = 64
        for sub in range(subs):
            for k in range(AXES):
                if phase == 4:
                    last_copy(i, sub, k, 0, 0).wait_recv()

                def add_rows(r, carry):
                    lo = pl.multiple_of(sub * count + r * group, group)
                    value = own_buf[s % 2, k, pl.ds(lo, group)].astype(jnp.float32) + pair_buf[s % 2, k, pl.ds(lo, group)].astype(jnp.float32)
                    for source in sources:
                        value = value + landed[source, k, pl.ds(base + lo, group)]
                    if phase < 4:
                        stage[k, slot, pl.ds(lo, group)] = value
                        return carry
                    for parity in range(2):
                        value = value + raw[k, parity, pl.ds(base + lo, group)].astype(jnp.float32)
                    value = value * (1.0 / devices)
                    landed[0, k, pl.ds(base + lo, group)] = value
                    return carry + jnp.sum((value * value).reshape(group // 8, 8, third), axis=0)

                if phase < 4:
                    lax.fori_loop(0, count // group, add_rows, 0)
                else:
                    part_buf[...] += lax.fori_loop(0, count // group, add_rows, jnp.zeros((8, third), jnp.float32))
                if phase < 3:
                    piece_copy(j, i, k, slot, (k + phase - 1) % AXES).start()
                elif phase == 3:
                    last_copy(i, sub, k, slot, (k + phase - 1) % AXES).start()
        if phase == 4:
            for k in range(AXES):
                pltpu.make_async_copy(
                    landed.at[0, k, pl.ds(base, part_rows)],
                    g_out.at[pl.ds(base, part_rows), pl.ds(k * third, third)], g_sem.at[k]).start()
        load_next()

    def pairs_sent(k):
        return pltpu.make_async_remote_copy(
            src_ref=pairs.at[:, k], dst_ref=pairs.at[:, k], send_sem=pair_ssem.at[k], recv_sem=pair_rsem.at[0, k],
            device_id=(partner,), device_id_type=MESH)

    part_buf[...] = jnp.zeros_like(part_buf)
    for phase, lo, hi in ((1, 0, 3), (2, 3, 5), (3, 5, 6), (4, 6, 7)):
        def run(s, carry, phase=phase):
            step(s, phase)
            return carry
        for source in ([], [0, 1], [2, 3], [4])[phase - 1]:
            for k in range(AXES):
                unit_recv(source, k).wait_recv()
        if phase == 4:
            for k in range(AXES):
                pairs_sent(k).wait_send()
            for k in range(AXES):
                for parity in range(2):
                    raw_recv(k, parity).wait_recv()
                    raw_copy(k, parity).wait_send()
        lax.fori_loop(lo * CHUNKS, hi * CHUNKS, run, 0)

    part_buf[:, :128] = part_buf[:, :128] + part_buf[:, 128:]
    norm_buf[me] = part_buf[:, :128]

    def norm_copy(d):
        return pltpu.make_async_remote_copy(
            src_ref=part_buf.at[:, pl.ds(0, 128)],
            dst_ref=norm_buf.at[me],
            send_sem=norm_sem.at[0],
            recv_sem=norm_sem.at[1],
            device_id=(bit_flip(me, d),),
            device_id_type=MESH)

    norm_all = pltpu.make_async_remote_copy(
        src_ref=norm_buf.at[pl.ds(1, devices - 1)], dst_ref=norm_buf.at[pl.ds(1, devices - 1)],
        send_sem=norm_sem.at[0], recv_sem=norm_sem.at[1], device_id=(partner,), device_id_type=MESH)

    for d in sorted(range(1, devices), key=lambda d: -bin(d // 2).count('1')):
        norm_copy(d).start()
    for last in range(SLOTS):
        for k in range(AXES):
            piece_copy(0, 0, k, last, 0).wait_send()
    for k in range(AXES):
        pltpu.make_async_copy(landed.at[0, k], g_out.at[:, pl.ds(k * third, third)], g_sem.at[k]).wait()
    norm_all.wait_send()
    norm_all.wait_recv()
    square_sum = jnp.sum(jnp.sum(norm_buf[...], axis=0), keepdims=True)
    c_out[...] = jnp.broadcast_to(jnp.minimum(1.0, 1.0 / (jnp.sqrt(square_sum) + 1e-6)), c_out.shape)


def reduce_scatter(local_grads, devices):
    total_rows, width = local_grads.shape[1:]
    rows, third = total_rows // devices, width // AXES
    any_spec = pl.BlockSpec(memory_space=pl.ANY)
    f32, bf16 = jnp.float32, jnp.bfloat16
    part_rows = rows // CHUNKS
    g, scale, _ = pl.pallas_call(
        reduce_kernel,
        out_shape=(jax.ShapeDtypeStruct((rows, width), f32),
                   jax.ShapeDtypeStruct((8, 128), f32),
                   jax.ShapeDtypeStruct((UNITS, AXES, rows, third), bf16)),
        in_specs=[any_spec],
        out_specs=(any_spec, pl.BlockSpec(memory_space=pltpu.VMEM), any_spec),
        scratch_shapes=[
            pltpu.VMEM((UNITS - 1, AXES, rows, third), f32),
            pltpu.VMEM((AXES, 2, rows, third), bf16),
            pltpu.VMEM((AXES, SLOTS, part_rows, third), f32),
            pltpu.VMEM((2, AXES, part_rows, third), bf16),
            pltpu.VMEM((2, AXES, part_rows, third), bf16),
            pltpu.VMEM((8, third), f32),
            pltpu.VMEM((devices, 8, 128), f32),
            pltpu.SemaphoreType.DMA((AXES,)),
            pltpu.SemaphoreType.DMA((PAIR_RING, AXES)),
            pltpu.SemaphoreType.DMA((AXES, SLOTS)),
            pltpu.SemaphoreType.DMA((UNITS - 2, AXES)),
            pltpu.SemaphoreType.DMA((AXES, CHUNKS, SUBS)),
            pltpu.SemaphoreType.DMA((2, AXES)),
            pltpu.SemaphoreType.DMA((2, AXES)),
            pltpu.SemaphoreType.DMA((AXES, 2)),
            pltpu.SemaphoreType.DMA((AXES, 2)),
            pltpu.SemaphoreType.DMA((2,)),
            pltpu.SemaphoreType.DMA((AXES,)),
        ],
        compiler_params=pltpu.CompilerParams(has_side_effects=True, vmem_limit_bytes=60 * 1024 * 1024, collective_id=0),
        name='reduce',
    )(local_grads)
    return g, scale


def update_gather_kernel(grad, master, first, second, scale, rate, working, new_master, new_first, new_second,
                         in_buf, out_buf, rate_buf, scale_buf, small_sem, in_sem, out_sem, own_ssem, own_rsem, fwd_ssem, fwd_rsem, pair_ssem, pair_rsem):
    me = lax.axis_index('dp')
    partner = bit_flip(me, 1)
    rows, width = grad.shape
    third = width // AXES
    total_rows = working.shape[0]
    pieces = rows // PIECE_ROWS
    inputs = (grad, master, first, second)

    def piece_at(owner, i, cols, piece_rows):
        return working.at[pl.ds(pl.multiple_of(owner * rows + i * piece_rows, piece_rows), piece_rows), cols]

    def first_send(t, axis):
        return send(me, t, every, own_ssem.at[axis], own_rsem.at[axis, 0], chip_flip(axis), LOAD_ROWS)

    def send(owner, i, cols, ssem, rsem, target, piece_rows=PIECE_ROWS):
        ref = piece_at(owner, i, cols, piece_rows)
        return pltpu.make_async_remote_copy(src_ref=ref, dst_ref=ref, send_sem=ssem, recv_sem=rsem,
                                            device_id=(target,), device_id_type=MESH)

    every = pl.ds(0, width)

    def cols_of(k):
        return pl.ds((k % AXES) * third, third)

    def chip_flip(*axes):
        mask = 0
        for axis in axes:
            mask ^= 2 << (axis % AXES)
        return bit_flip(me, mask)

    def load(t, n):
        here = pl.ds(pl.multiple_of(t * LOAD_ROWS, LOAD_ROWS), LOAD_ROWS)
        return pltpu.make_async_copy(inputs[n].at[here], in_buf.at[t % LOADS, n], in_sem.at[t % LOADS, n])

    def store(t):
        here = pl.ds(pl.multiple_of(t * LOAD_ROWS, LOAD_ROWS), LOAD_ROWS)
        return pltpu.make_async_copy(out_buf.at[t % 2], new_second.at[here], out_sem.at[t % 2])

    def own_send(i, axis):
        return send(me, i, every, own_ssem.at[axis], own_rsem.at[axis, i], chip_flip(axis))

    def own_recv(i, axis):
        return send(chip_flip(axis), i, every, own_ssem.at[axis], own_rsem.at[axis, i], chip_flip(axis))

    fwd_base = [AXES * sum(rows // n for n in FORWARD_ROWS[:kind]) for kind in range(4)]
    hops = (((0,), 1), ((0,), 2), ((1,), 2), ((0, 1), 2))

    def fwd_send(i, kind, k):
        source, axis = hops[kind]
        return send(chip_flip(*[k + a for a in source]), i, cols_of(k), fwd_ssem.at[kind], fwd_rsem.at[fwd_base[kind] + k * (rows // FORWARD_ROWS[kind]) + i], chip_flip(k + axis), FORWARD_ROWS[kind])

    def fwd_recv(i, kind, k):
        source, axis = hops[kind]
        return send(chip_flip(*[k + a for a in source], k + axis), i, cols_of(k), fwd_ssem.at[kind], fwd_rsem.at[fwd_base[kind] + k * (rows // FORWARD_ROWS[kind]) + i], chip_flip(k + axis), FORWARD_ROWS[kind])

    def pair_own(i):
        return send(me, i, every, pair_ssem.at[0], pair_rsem.at[0], partner)

    def pair_axis(i, axis):
        return send(chip_flip(axis), i, every, pair_ssem.at[1 + axis], pair_rsem.at[1 + axis], partner)

    def pair_fwd(i, kind, k):
        source, axis = hops[kind]
        owner = chip_flip(*[k + a for a in source], k + axis)
        return send(owner, i, cols_of(k), pair_ssem.at[4 + kind], pair_rsem.at[4 + kind], partner, FORWARD_ROWS[kind])

    def whole(ssem, rsem):
        return send(me, 0, every, ssem, rsem, partner, rows)

    run_starts, lr_values, decay_values = layout_runs(width, total_rows)
    first_norm = 1.0 / (1.0 - 0.9 ** ADAM_STEP)
    second_norm = 1.0 / (1.0 - 0.99 ** ADAM_STEP)

    steps = rows // LOAD_ROWS
    small = (pltpu.make_async_copy(scale, scale_buf, small_sem.at[0]), pltpu.make_async_copy(rate, rate_buf, small_sem.at[1]))
    for copy in small:
        copy.start()
    barrier = pltpu.get_barrier_semaphore()
    peers = [partner] + [chip_flip(axis) for axis in range(AXES)]
    for peer in peers:
        pl.semaphore_signal(barrier, inc=1, device_id=(peer,), device_id_type=MESH)
    for t in range(LOADS):
        for n in range(4):
            load(t, n).start()
    def update_rows(t, carry):
        for n in range(4):
            load(t, n).wait()

        @pl.when(t >= 2)
        def _():
            store(t - 2).wait()
        slot = t % LOADS
        out_slot = t % 2
        group = 16

        def group_step(r, carry):
            lo = pl.multiple_of(r * group, group)
            here = pl.ds(lo, group)
            row = pl.multiple_of(t * LOAD_ROWS + lo, group)
            start = me * rows + row
            row_ids = start + lax.broadcasted_iota(jnp.int32, (group, 128), 0)
            factor = jnp.full((group, 128), lr_values[0], jnp.float32)
            decay = jnp.full((group, 128), decay_values[0], jnp.float32)
            for r_start, r_lr, r_decay in zip(run_starts[1:], lr_values[1:], decay_values[1:]):
                past = row_ids >= r_start
                factor = jnp.where(past, r_lr, factor)
                decay = jnp.where(past, r_decay, decay)
            step_size = rate_buf[...] * factor
            for tile in range(width // 128):
                at = pl.ds(tile * 128, 128)
                clipped = in_buf[slot, 0, here, at] * scale_buf[pl.ds(0, 1)]
                weights = in_buf[slot, 1, here, at]
                moment = 0.9 * in_buf[slot, 2, here, at] + 0.1 * clipped
                square = 0.99 * in_buf[slot, 3, here, at] + 0.01 * (clipped * clipped)
                moved = weights - step_size * ((moment * first_norm) / (jnp.sqrt(square * second_norm) + 1e-8) + decay * weights)
                new_master[pl.ds(row, group), at] = moved
                new_first[pl.ds(row, group), at] = moment
                out_buf[out_slot, here, at] = square
                working[pl.ds(pl.multiple_of(start, group), group), at] = moved.astype(jnp.bfloat16)
            return carry

        lax.fori_loop(0, LOAD_ROWS // group, group_step, 0)
        store(t).start()

        @pl.when(t + LOADS < steps)
        def _():
            for n in range(4):
                load(t + LOADS, n).start()
        return carry

    def own_piece(i, carry):
        per = PIECE_ROWS // LOAD_ROWS
        lax.fori_loop(i * per, (i + 1) * per, update_rows, 0)
        for axis in range(AXES):
            own_send(i, axis).start()
        pair_own(i).start()
        return carry

    def neighbour_piece(i, carry):
        per = FORWARD_ROWS[0] // PIECE_ROWS
        for part in range(per):
            for axis in range(AXES):
                own_recv(i * per + part, axis).wait_recv()
                pair_axis(i * per + part, axis).start()
        for kind in range(3):
            for k in range(AXES):
                fwd_send(i, kind, k).start()
        return carry

    def far_piece(i, carry):
        per = FORWARD_ROWS[0] // FORWARD_ROWS[3]
        for k in range(AXES):
            fwd_recv(i, 0, k).wait_recv()
            for part in range(per):
                fwd_send(i * per + part, 3, k).start()
            pair_fwd(i, 0, k).start()
        for kind in (1, 2):
            for k in range(AXES):
                fwd_recv(i, kind, k).wait_recv()
                pair_fwd(i, kind, k).start()
        return carry

    def last_piece(i, carry):
        for k in range(AXES):
            fwd_recv(i, 3, k).wait_recv()
            pair_fwd(i, 3, k).start()
        return carry

    def drain_own():
        for axis in range(AXES):
            whole(own_ssem.at[axis], own_rsem.at[axis, 0]).wait_send()
        for slot in range(4):
            whole(pair_ssem.at[slot], pair_rsem.at[slot]).wait_send()
            whole(pair_ssem.at[slot], pair_rsem.at[slot]).wait_recv()

    def drain_fwd(kinds):
        for kind in kinds:
            whole(fwd_ssem.at[kind], fwd_rsem.at[fwd_base[kind]]).wait_send()
            whole(pair_ssem.at[4 + kind], pair_rsem.at[4 + kind]).wait_send()
            whole(pair_ssem.at[4 + kind], pair_rsem.at[4 + kind]).wait_recv()

    near_pieces, far_pieces = rows // FORWARD_ROWS[0], rows // FORWARD_ROWS[3]
    for copy in small:
        copy.wait()
    for t in range(PIECE_ROWS // LOAD_ROWS):
        update_rows(t, 0)
        if t == 0:
            pl.semaphore_wait(barrier, len(peers))
        for axis in range(AXES):
            first_send(t, axis).start()
    pair_own(0).start()
    lax.fori_loop(1, pieces, own_piece, 0)
    lax.fori_loop(0, near_pieces, neighbour_piece, 0)
    for t in (steps - 2, steps - 1):
        store(t).wait()
    drain_own()
    lax.fori_loop(0, near_pieces, far_piece, 0)
    drain_fwd((0, 1, 2))
    lax.fori_loop(0, far_pieces, last_piece, 0)
    drain_fwd((3,))


def write_kernel(working, new_master, new_first, new_second, working_out, master_out, first_out, second_out,
                 buf, put_sem, in_sem, out_sem):
    rows = new_second.shape[0]
    slots, piece = buf.shape[:2]
    steps = rows // piece

    def load(s):
        return pltpu.make_async_copy(new_second.at[pl.ds(s * piece, piece)], buf.at[s % slots], in_sem.at[s % slots])

    def store(s):
        return pltpu.make_async_copy(buf.at[s % slots], second_out.at[pl.ds(s * piece, piece)], out_sem.at[s % slots])

    puts = [pltpu.make_async_copy(new_master, master_out, put_sem.at[0]), pltpu.make_async_copy(new_first, first_out, put_sem.at[1])]
    stripes = put_sem.shape[0] - 2
    stripe = working.shape[0] // stripes
    for n in range(stripes):
        here = pl.ds(n * stripe, stripe)
        puts.append(pltpu.make_async_copy(working.at[here], working_out.at[here], put_sem.at[n + 2]))

    for s in range(slots):
        load(s).start()
    for s in range(steps):
        for put in puts[s * len(puts) // steps:(s + 1) * len(puts) // steps]:
            put.start()
        load(s).wait()
        store(s).start()
        if s + 1 >= slots and s + 1 < steps:
            store(s + 1 - slots).wait()
            load(s + 1).start()
    for s in range(steps - slots, steps):
        store(s).wait()
    for put in puts:
        put.wait()


def update_gather(grad, master, first, second, scale, rate, devices):
    rows, width = grad.shape
    any_spec = pl.BlockSpec(memory_space=pltpu.HBM)
    vmem_spec = pl.BlockSpec(memory_space=pltpu.VMEM)
    f32, bf16 = jnp.float32, jnp.bfloat16
    pieces = rows // PIECE_ROWS
    shard = pltpu.HBM((rows, width), f32)
    near = pltpu.VMEM((rows, width), f32)
    dma = pltpu.SemaphoreType.DMA
    working, new_master, new_first, new_second = pl.pallas_call(
        update_gather_kernel,
        out_shape=(pltpu.VMEM((devices * rows, width), bf16), near, near, shard),
        in_specs=[any_spec] * 6,
        out_specs=(vmem_spec, vmem_spec, vmem_spec, any_spec),
        scratch_shapes=[
            pltpu.VMEM((LOADS, 4, LOAD_ROWS, width), f32),
            pltpu.VMEM((2, LOAD_ROWS, width), f32),
            pltpu.VMEM((1, 128), f32),
            pltpu.VMEM((8, 128), f32),
            dma((2,)),
            dma((LOADS, 4)),
            dma((2,)),
            dma((AXES,)),
            dma((AXES, pieces)),
            dma((4,)),
            dma((AXES * sum(rows // n for n in FORWARD_ROWS),)),
            dma((8,)),
            dma((8,)),
        ],
        compiler_params=pltpu.CompilerParams(has_side_effects=True, vmem_limit_bytes=3 * 1024 * 1024, collective_id=1),
        name='gather',
    )(grad, master, first, second, scale, jnp.broadcast_to(rate, (1, 128)))
    working_shape = pltpu.HBM((devices * rows, width), bf16)
    return pl.pallas_call(
        write_kernel,
        out_shape=(working_shape, shard, shard, shard),
        in_specs=[vmem_spec, vmem_spec, vmem_spec, any_spec],
        out_specs=(any_spec,) * 4,
        scratch_shapes=[pltpu.VMEM((3, rows // 8, width), f32), dma((18,)), dma((3,)), dma((3,))],
        compiler_params=pltpu.CompilerParams(vmem_limit_bytes=3 * 1024 * 1024),
        name='write',
    )(*[pltpu.with_memory_space_constraint(x, pltpu.VMEM) for x in (working, new_master, new_first)], new_second)


def solution(mesh):
    dev_count = mesh.shape['dp']

    def device_step(local_grads, master, mom_first, mom_second, learn_rate):
        grad_shard, clip_scale = reduce_scatter(local_grads, dev_count)
        working, new_master, new_first, new_second = update_gather(grad_shard, master, mom_first, mom_second, clip_scale, learn_rate, dev_count)
        return new_master, new_first, new_second, working

    return jax.shard_map(device_step, mesh=mesh, in_specs=(P('dp', None, None), P('dp', None), P('dp', None), P('dp', None), P()), out_specs=(P('dp', None), P('dp', None), P('dp', None), P(None, None)), check_vma=False)
```
